32 devices in a mesh: gx: 8 (over z, y), gy: 4 (over x, core).
Axes of the slice: x: 2, y: 2, z: 4, core: 2. Of those that a mesh axis runs over, the one named last changes fastest.
Arguments:
- vorticity_grid: float32 [4096, 4096], P(('gx', 'gy')), may hold values from -6 to 6
- forcing_grid: float32 [4096, 4096], P(('gx', 'gy')), may hold values from -12 to 12
- cutoff: int32 [1], replicated, may hold values from 853 to 1365
- forcing_shells: int32 [4], replicated, may hold values from 2 to 127
Outputs:
- lifted_spectrum: float32 [2, 4096, 4096], P(None, ('gx', 'gy'))
- coarse_field: float32 [256, 256], P(('gx', 'gy'))
The draws below stay inside these ranges and needn't reach their ends.
Inputs may be any that keep to these rules, and one draw needn't show every extreme that they name: Nonlinear modes with an absolute wavenumber index above cutoff are removed.
All inputs are finite; a program needn't handle non-finite values.
Results may differ from the reference program's by a relative error of at most 0.0001.
Values sent between devices are 32-bit elements; how exact they have to be, the bound alone decides.
A program may use at most 128 MiB of HBM per device.

```python
import math
import jax
import jax.numpy as jnp

GRID = 4096
STEPS = 1
LOW = 256
SHELLS = 4


def with_ends(array, rng, least, high):
    longest = array.shape.index(max(array.shape))
    spots = []
    for shift in (0, 1):
        where = [jax.random.randint(jax.random.fold_in(rng, axis), (), 0, length) for axis, length in enumerate(array.shape)]
        where[longest] = (where[longest] + shift) % array.shape[longest]
        spots.append(tuple(where))
    return array.at[spots[0]].set(least).at[spots[1]].set(high)


def levels(rng, shape, shards, least, high):
    loudness, own = 1.0, jax.random.fold_in(rng, 6)
    for position, shards_of in shards:
        steps = jnp.exp(jax.random.uniform(jax.random.fold_in(own, position), (shards_of,), jnp.float32, least / len(shards), high / len(shards)))
        loudness = loudness * jnp.repeat(steps, shape[position] // shards_of).reshape([-1 if axis == position else 1 for axis in range(len(shape))])
    return loudness


def centred(rng, shape, deviation, reach, cuts=(), kind=jnp.bfloat16):
    factor_of = levels(rng, shape, cuts, -0.22, 0.18) if cuts else 1.0
    values = jax.random.normal(rng, shape, jnp.float32) * deviation * factor_of
    return jnp.minimum(jnp.maximum(values, -reach), reach).astype(kind)


def setup_inputs(seed: int = 0) -> dict:
    keys = jax.random.split(jax.random.key(seed), 5)
    vorticity_grid = centred(keys[0], (GRID, GRID), 1.0, 6.0, ((0, 32),), jnp.float32)
    forcing_grid = centred(keys[1], (GRID, GRID), 2.0, 12.0, ((0, 32),), jnp.float32)
    cutoff = jax.random.randint(keys[2], (1,), GRID // 3 - GRID // 8, GRID // 3 + 1).astype(jnp.int32)
    forcing_shells = with_ends(jax.random.randint(keys[3], (SHELLS,), 2, LOW // 2), jax.random.fold_in(keys[3], 1), 2, (LOW // 2) - 1).astype(jnp.int32)
    return dict(vorticity_grid=vorticity_grid, forcing_grid=forcing_grid, cutoff=cutoff, forcing_shells=forcing_shells)


time_step = 0.05
viscosity = 0.05
coarse_ratio = 4.0


def signed_index(index_array, length_of):
    return jnp.where(index_array < length_of // 2, index_array, index_array - length_of)


def to_spectrum(physical):
    return jnp.fft.fft2(physical, norm="ortho").T


def to_grid(spectrum):
    return jnp.fft.ifft2(spectrum.T, norm="ortho")


def reference(vorticity_grid, forcing_grid, cutoff, forcing_shells):
    indices = jnp.arange(GRID, dtype=jnp.int32)
    wave_y = signed_index(indices, GRID)[:, None]
    wave_x = signed_index(indices, GRID)[None, :]
    wave_unit = 2.0 * math.pi / GRID
    deriv_y = jnp.where(indices[:, None] == GRID // 2, 0, wave_y).astype(jnp.float32) * wave_unit
    deriv_x = jnp.where(indices[None, :] == GRID // 2, 0, wave_x).astype(jnp.float32) * wave_unit
    squares = wave_x * wave_x + wave_y * wave_y
    laplace = squares.astype(jnp.float32) * (wave_unit * wave_unit)
    inverse_lap = jnp.where(squares == 0, 0.0, 1.0 / jnp.maximum(laplace, wave_unit * wave_unit))
    dealias = (jnp.abs(wave_x) <= cutoff[0]) & (jnp.abs(wave_y) <= cutoff[0])
    shell_mask = jnp.zeros((GRID, GRID), dtype=bool)
    for shell_index in range(SHELLS):
        radius = forcing_shells[shell_index]
        shell_mask = shell_mask | ((radius * radius <= squares) & (squares < (radius + 1) * (radius + 1)))
    drive = jnp.where(shell_mask, to_spectrum(forcing_grid), 0.0)
    vorticity = to_spectrum(vorticity_grid)

    def tendency(state):
        stream = state * inverse_lap
        velocity_u = to_grid(1j * deriv_y * stream).real
        velocity_v = to_grid(-1j * deriv_x * stream).real
        grad_x = to_grid(1j * deriv_x * state).real
        grad_y = to_grid(1j * deriv_y * state).real
        advect = velocity_u * grad_x + velocity_v * grad_y
        nonlinear = jnp.where(dealias, to_spectrum(advect), 0.0)
        return -nonlinear - viscosity * laplace * state + drive

    earlier = vorticity
    for step_index in range(STEPS):
        earlier = vorticity
        first_slope = tendency(vorticity)
        second_slope = tendency(vorticity + time_step * first_slope)
        vorticity = vorticity + 0.5 * time_step * (first_slope + second_slope)
    projected = vorticity + coarse_ratio * (vorticity - earlier)
    half_low = LOW // 2
    low_modes = (wave_x >= -half_low) & (wave_x < half_low) & (wave_y >= -half_low) & (wave_y < half_low)
    lifted = jnp.where(low_modes, projected, vorticity)
    block_rows = jnp.concatenate([projected[:half_low], projected[GRID - half_low:]], axis=0)
    block_low = jnp.concatenate([block_rows[:, :half_low], block_rows[:, GRID - half_low:]], axis=1)
    coarse = jnp.fft.ifft2(block_low.T, norm="ortho").real
    return jnp.stack([lifted.real, lifted.imag]), coarse
```

```python
import functools
import math

import jax
import jax.numpy as jnp
import numpy as np
from jax import lax
from jax.experimental import pallas as pl
from jax.experimental.pallas import tpu as pltpu
from jax.sharding import PartitionSpec as P

LOW = 256
SHELLS = 4
AXES = ("gx", "gy")

time_step = 0.05
viscosity = 0.05
coarse_ratio = 4.0


def contract(pattern, left_side, right_side):
    return jnp.einsum(pattern, left_side, right_side, precision=lax.Precision.HIGH)


def turn(product, length_of):
    phases = 2.0 * np.pi / length_of * (product % length_of)
    return np.cos(phases), np.sin(phases)


def rotation(cos_part, sin_part, axes):
    pairs = np.stack([np.stack([cos_part, -sin_part]), np.stack([sin_part, cos_part])])
    return np.moveaxis(pairs, (0, 1), axes).astype(np.float32)


def wave_tables(grid, total, rows):
    own = total // 2
    scale = 1.0 / math.sqrt(grid)
    t, a = np.arange(rows), np.arange(rows)
    b, D = np.arange(total), np.arange(total)
    out = {}
    cos_t, sin_t = turn(t[:, None] * a[None, :], rows)
    out["y1"] = np.stack([cos_t, -sin_t], 1).astype(np.float32)
    out["iy1"] = np.moveaxis(np.stack([cos_t, -sin_t], 1), 2, 0).astype(np.float32)
    ky = rows * D[None, :, None] + t[:, None, None]
    cos_t, sin_t = turn(ky * b[None, None, :], grid)
    sign = 1.0 - 2.0 * (b % 2)
    table = np.moveaxis(rotation(cos_t * scale, -sin_t * scale, (0, 1)), (0, 1), (2, 3))
    out["y2_low"] = table.copy()
    table[0, 0, 1] = np.stack([sign * scale, 0 * sign])
    table[0, own, 1] = np.stack([0 * sign + scale, 0 * sign])
    out["y2"] = table
    cos_t, sin_t = np.moveaxis(cos_t[:, :own], 1, 2), np.moveaxis(sin_t[:, :own], 1, 2)
    weight = np.where(ky[:, None, :own, 0] == 0, scale, 2.0 * scale)
    back = np.moveaxis(rotation(cos_t * weight, sin_t * weight, (0, 1)), (0, 1), (1, 4))
    back[0, :, :, 0, 1] = np.stack([sign * scale, 0 * sign])
    out["iy"] = back
    slope = np.moveaxis(rotation(-sin_t * weight, cos_t * weight, (0, 1)), (0, 1), (1, 4))
    slope[0, :, :, 0, :] = 0.0
    out["iyd"] = slope
    p, s = np.arange(total), np.arange(total)
    q, lane = np.arange(rows), np.arange(rows)
    cos_t, sin_t = turn(p[:, None] * s[None, :], total)
    out["x1"] = rotation(cos_t * scale, -sin_t * scale, (1, 3))
    cos_t, sin_t = turn(s[:own, None] * p[None, :], total)
    out["ix1"] = rotation(cos_t * scale, sin_t * scale, (1, 3))
    cos_t, sin_t = turn(q[:, None] * lane[None, :], rows)
    out["x2"] = rotation(cos_t.T, -sin_t.T, (2, 0))
    out["ix2"] = rotation(cos_t, sin_t, (2, 0))
    cos_t, sin_t = turn(p[:, None] * lane[None, :], grid)
    out["tw"] = np.stack([cos_t, sin_t]).astype(np.float32)
    return out


TILE = 16
PART = 32


def plus(one, two, sign=1.0):
    if two is None:
        return one
    if one is None:
        return tuple(sign * part for part in two)
    if sign > 0:
        return one[0] + two[0], one[1] + two[1]
    return one[0] - two[0], one[1] - two[1]


def turned_by(value, step, length, sign):
    if value is None:
        return None
    step = step % length
    real, imag = value
    if step == 0:
        return value
    if 2 * step == length:
        return -real, -imag
    if 4 * step == length:
        return (-imag, real) if sign > 0 else (imag, -real)
    if 4 * step == 3 * length:
        return (imag, -real) if sign > 0 else (-imag, real)
    angle = 2.0 * math.pi * step / length
    c, s = math.cos(angle), sign * math.sin(angle)
    return real * c - imag * s, real * s + imag * c


def small_fft(values, sign):
    size = len(values)
    if size == 1:
        return values
    even, odd = small_fft(values[::2], sign), small_fft(values[1::2], sign)
    odd = [turned_by(value, k, size, sign) for k, value in enumerate(odd)]
    return [plus(e, o) for e, o in zip(even, odd)] + [plus(e, o, -1.0) for e, o in zip(even, odd)]


def long_fft(total, load, store, between, sign, side=None):
    wide = 4
    deep = total // wide
    for j in range(deep):
        out = small_fft([load(deep * i + j) for i in range(wide)], sign)
        for u in range(wide):
            real, imag = turned_by(out[u], j * u, total, sign)
            between[u * deep + j, 0] = real
            between[u * deep + j, 1] = imag
    for u in range(wide):
        values = [(between[u * deep + j, 0], between[u * deep + j, 1]) for j in range(deep)]
        if side is None:
            for v, value in enumerate(small_fft(values, sign)):
                store(u + wide * v, value)
        else:
            even, odd = small_fft(values[::2], sign), small_fft(values[1::2], sign)
            for v in range(deep // 2):
                o = turned_by(odd[v], v, deep, sign)
                store(u + wide * v, (even[v][0] + side * o[0], even[v][1] + side * o[1]))


def split(value):
    high = value.astype(jnp.bfloat16)
    return high, (value - high.astype(jnp.float32)).astype(jnp.bfloat16)


def halves_of(table):
    table = np.asarray(table, np.float32)
    high = table.astype(jnp.bfloat16)
    return high, (table - high.astype(np.float32)).astype(jnp.bfloat16)


def dot3(left, right):
    def dot(a, b):
        return jnp.dot(a, b, preferred_element_type=jnp.float32)

    return dot(left[0], right[0]) + dot(left[1], right[0]) + dot(left[0], right[1])


def y_tables(grid, total, rows):
    scale = 1.0 / math.sqrt(grid)
    b, t, a = np.arange(total)[:, None, None], np.arange(rows)[None, :, None], np.arange(rows)
    cos_t, sin_t = turn(t * a * total + t * b, grid)
    forth = np.concatenate([cos_t, -sin_t], 1) * scale
    return forth, 2.0 * forth.transpose(0, 2, 1)


def x_tables(grid, total, rows):
    scale = 1.0 / math.sqrt(grid)
    l, q = np.arange(rows)[:, None], np.arange(rows)[None, :]
    cos_t, sin_t = turn(l * q, rows)
    forth = np.block([[cos_t, -sin_t], [sin_t, cos_t]]) * scale
    back = np.block([[cos_t, sin_t], [-sin_t, cos_t]]) * scale
    cos_t, sin_t = turn(np.arange(total)[:, None] * np.arange(rows)[None, :], grid)
    return forth, back, np.stack([cos_t, sin_t], 1).astype(np.float32)[:, :, None, :]


def params():
    return pltpu.CompilerParams(vmem_limit_bytes=56 * 1024 * 1024)


def forward_rows(total, rows, waves, out_ref, between):
    def tile(i, carry):
        spot = pl.ds(pl.multiple_of(i * TILE, TILE), TILE)
        low = pl.ds(pl.multiple_of(rows + i * TILE, TILE), TILE)

        def store(D, value):
            out_ref[D, 0, spot, :] = value[0]
            out_ref[D, 1, spot, :] = value[1]

        long_fft(total, lambda b: (waves[b, spot, :], waves[b, low, :]), store, between, -1.0)
        return carry

    lax.fori_loop(0, rows // TILE, tile, 0)
    top = pl.ds(0, 8)
    here = lax.broadcasted_iota(jnp.int32, (8, rows), 0) == 0
    middle = total // 2
    zero, other = out_ref[0, 0, top, :], out_ref[middle, 0, top, :]
    out_ref[0, 1, top, :] = jnp.where(here, other, out_ref[0, 1, top, :])
    out_ref[middle, 1, top, :] = jnp.where(here, zero, out_ref[middle, 1, top, :])


def start_kernel(total, rows, field, forth_hi, forth_lo, out_ref, waves, between):
    def step(b, carry):
        waves[b] = dot3((forth_hi[b], forth_lo[b]), split(field[b]))
        return carry

    lax.fori_loop(0, total, step, 0)
    forward_rows(total, rows, waves, out_ref, between)


def product_kernel(total, rows, unit, info, forth_hi, forth_lo, back_hi, back_lo, *refs):
    fields, out_ref, waves, left, right, between = refs[0], *refs[-5:]
    psi, psi_x, vort_x = (fields.at[:, i] for i in range(3))
    vort = fields.at[:, 3] if len(refs) == 6 else refs[1]
    own = total // 2
    offset = info[3]

    def waves_of(field, slope, begin):
        def tile(i, carry):
            spot = pl.ds(pl.multiple_of(i * TILE, TILE), TILE)
            top = pl.ds(pl.multiple_of(begin + i * TILE, TILE), TILE)
            low = pl.ds(pl.multiple_of(begin + rows + i * TILE, TILE), TILE)
            row = lax.broadcasted_iota(jnp.int32, (TILE, rows), 0) + (i * TILE + begin)
            here = row == 0

            def load(r):
                if r > own or (r == own and slope):
                    return None
                if r == own:
                    imag = field[0, 1, spot, :]
                    return jnp.where(here, 0.5 * imag, 0.0), jnp.zeros_like(imag)
                real, imag = field[r, 0, spot, :], field[r, 1, spot, :]
                if slope:
                    factor = (row + (r * rows - offset)).astype(jnp.float32) * unit
                    if r == 0:
                        factor = jnp.where(here, 0.0, factor)
                    return -factor * imag, factor * real
                if r == 0:
                    real = jnp.where(here, 0.5 * real, real)
                    imag = jnp.where(here, 0.0, imag)
                return real, imag

            def store(b, value):
                waves[b, top, :] = value[0]
                waves[b, low, :] = value[1]

            long_fft(total, load, store, between, 1.0)
            return carry

        lax.fori_loop(0, rows // TILE, tile, 0)

    def physical(b):
        return dot3((back_hi[b], back_lo[b]), split(waves[b]))

    def each(step):
        def run(b, carry):
            step(b)
            return carry

        lax.fori_loop(0, total, run, 0)

    def first(b):
        left[b] = physical(b)

    def second(b):
        left[b] = left[b] * physical(b)

    def third(b):
        right[b] = physical(b)

    def fourth(b):
        advect = left[b] - right[b] * physical(b)
        waves[b] = dot3((forth_hi[b], forth_lo[b]), split(advect))

    for field, slope, step in (
        (psi, True, first), (vort_x, False, second), (psi_x, False, third), (vort, True, fourth),
    ):
        waves_of(field, slope, 0)
        each(step)
    forward_rows(total, rows, waves, out_ref, between)


def spectral_kernel(total, rows, grid, stage, *refs):
    refs = list(refs)

    def take(count):
        out = refs[:count]
        del refs[:count]
        return out

    info, side_of, source, twist, forth_hi, forth_lo, back_hi, back_lo = take(8)
    state_in = take(1)[0] if stage > 0 else None
    moved_in, first_in = take(2) if stage == 2 else (None, None)
    drive_in = take(1)[0] if stage > 0 else None
    state_out = take(1)[0] if stage == 0 else None
    moved_out, first_out = take(2) if stage == 1 else (None, None)
    ahead_out, now_out = take(2) if stage == 2 else (None, None)
    counted = 3 + stage if stage < 2 else 0
    landed = take(1)[0] if counted else None
    ins, outs, between, kept, arrived, sent_sem, come_sem, own_sem = take(8)
    room, field_sent, field_come, field_own = take(4) if counted else [None] * 4
    extra_first = True
    unit = 2.0 * math.pi / grid
    step = pl.program_id(0)
    riding = step == 0
    width = lax.axis_size("gy")
    me = lax.axis_index("gx") * width + lax.axis_index("gy")
    own = total // 2
    base = (me // own) * own
    slot = me - base
    reach = total if stage == 0 else (grid // 3) // rows
    parts = rows // PART

    def near(device):
        return (device <= reach) | (device >= total - 1 - reach)

    def place(device):
        return (device // width, device % width)

    def move(part, k, extent):
        dest = (me + k) % total
        spot = pl.ds(pl.multiple_of(part * PART, PART), extent)
        return pltpu.make_async_remote_copy(
            src_ref=source.at[dest, :, spot, :],
            dst_ref=arrived.at[me, :, spot, :],
            send_sem=sent_sem.at[part, k],
            recv_sem=come_sem.at[part],
            device_id=place(dest),
            device_id_type=pl.DeviceIdType.MESH,
        )

    def all_moves(act):
        def run(n, carry):
            part, k = n // (total - 1), n % (total - 1) + 1
            dest = (me + k) % total

            @pl.when(near(dest))
            def _():
                act(move(part, k, PART))

            if reach < own:

                @pl.when((dest == own) & (part == 0))
                def _():
                    act(move(part, k, TILE))

            return carry

        lax.fori_loop(0, parts * (total - 1), run, 0)

    mine = pltpu.make_async_copy(source.at[me], arrived.at[me], own_sem.at[0])

    def await_part(part, extent):
        spot = pl.ds(pl.multiple_of(part * PART, PART), extent)
        ref = arrived.at[pl.ds(0, total - 1), :, spot, :]
        pltpu.make_async_copy(ref, ref, come_sem.at[part]).wait()

    @pl.when(riding)
    def _():
        all_moves(lambda copy: copy.start())
        mine.start()
        mine.wait()

        if reach < own:

            @pl.when(me == own)
            def _():
                await_part(0, TILE)

    every = PART // TILE

    @pl.when(near(me) & (riding | ((step > 1) & ((step - 1) % every == 0))))
    def _():
        await_part(jnp.maximum(step - 1, 0) // every, PART)

    spot_in = pl.ds(pl.multiple_of(jnp.maximum(step - 1, 0) * TILE, TILE), TILE)
    origin = info[2] == 1
    tile = step - 1
    size = TILE
    shape = (size, rows)
    row = lax.broadcasted_iota(jnp.int32, shape, 0)
    first_here = (row == 0) & (tile == 0) & origin if extra_first else None
    side = side_of[0]

    def block(p):
        return pl.ds(pl.multiple_of(p * size, size), size)

    def load(s):
        real, imag = arrived[s, 0, spot_in, :], arrived[s, 1, spot_in, :]
        if extra_first:
            ride = jnp.where(row == 0, imag, 0.0)
            imag = jnp.where(riding | first_here, 0.0, imag)
            real = jnp.where(riding, ride, real)
        return real, imag

    def store(p, value):
        c, s = twist[p, 0], twist[p, 1]
        ins[p * size : (p + 1) * size, :rows] = value[0] * c + value[1] * s
        ins[p * size : (p + 1) * size, rows:] = value[1] * c - value[0] * s

    long_fft(total, load, store, between, -1.0)
    chunk = 8 * size

    def multiply(hi, lo):
        def run(i, carry):
            spot = pl.ds(pl.multiple_of(i * chunk, chunk), chunk)
            outs[spot, :] = dot3(split(ins[spot, :]), (hi[...], lo[...]))
            return carry

        lax.fori_loop(0, total * size // chunk, run, 0)

    multiply(forth_hi, forth_lo)
    wave_y = info[0] + tile * size + row
    if extra_first:
        wave_y = jnp.where(riding, info[1], wave_y)
    q = lax.broadcasted_iota(jnp.int32, shape, 1)
    cutoff = info[4]
    rows_kept = jnp.abs(wave_y) <= cutoff
    y_squared = wave_y * wave_y

    def waves_x(p):
        kx = p + total * q
        wave = jnp.where(kx < grid // 2, kx, kx - grid)
        slope = jnp.where(kx == grid // 2, 0, wave).astype(jnp.float32) * unit
        return wave, slope

    def squares_of(wave):
        squares = wave * wave + y_squared
        return squares, squares.astype(jnp.float32) * (unit * unit)

    def pair(ref, p):
        return ref[p, 0], ref[p, 1]

    def put(ref, p, value):
        ref[p, 0] = value[0]
        ref[p, 1] = value[1]

    step_size = time_step * viscosity

    def settle(p, carry):
        wave, _ = waves_x(p)
        squares, lap = squares_of(wave)
        found = outs[block(p), :rows], outs[block(p), rows:]
        if stage == 0:
            put(state_out, p, found)
            return carry
        mask = rows_kept & (jnp.abs(wave) <= cutoff)
        term = tuple(d - jnp.where(mask, part, 0.0) for d, part in zip(pair(drive_in, p), found))
        state = pair(state_in, p)
        if stage == 1:
            put(first_out, p, term)
            put(moved_out, p, tuple(s - step_size * lap * s + time_step * t for s, t in zip(state, term)))
            return carry
        low = LOW // 2
        inside = (wave >= -low) & (wave < low) & (wave_y >= -low) & (wave_y < low)
        moved, first = pair(moved_in, p), pair(first_in, p)
        for c in (0, 1):
            linear = viscosity * lap * (state[c] + moved[c])
            now = state[c] + 0.5 * time_step * (first[c] + term[c] - linear)
            ahead = now + coarse_ratio * (now - state[c])
            ahead_out[p, c] = ahead
            now_out[p, c] = jnp.where(inside, ahead, now)
        return carry

    lax.fori_loop(0, total, settle, 0)
    whole = state_out if stage == 0 else moved_out

    for index in range(counted):

        def fill(p, carry):
            wave, slope = waves_x(p)
            real, imag = pair(whole, p)
            if index < 2:
                squares, lap = squares_of(wave)
                inverse = jnp.where(squares == 0, 0.0, 1.0 / jnp.maximum(lap, unit * unit))
                real, imag = inverse * real, inverse * imag
            if index in (1, 2):
                real, imag = -slope * imag, slope * real
            ins[block(p), :rows] = real
            ins[block(p), rows:] = imag
            return carry

        lax.fori_loop(0, total, fill, 0)
        multiply(back_hi, back_lo)

        def load_back(p):
            real, imag = outs[p * size : (p + 1) * size, :rows], outs[p * size : (p + 1) * size, rows:]
            c, s = twist[p, 0], twist[p, 1]
            return real * c - imag * s, imag * c + real * s

        def store_back(s, value):
            real, imag = value
            if extra_first:
                imag = jnp.where(first_here, kept[index, s], imag)
                kept[index, s] = real
            room[s, index, 0, spot_in, :] = real
            room[s, index, 1, spot_in, :] = imag

        long_fft(total, load_back, store_back, between, 1.0, side)

    if counted:

        def field_move(i, k):
            spot = pl.ds(pl.multiple_of(i * TILE, TILE), TILE)
            to = (slot + k) % own
            return pltpu.make_async_remote_copy(
                src_ref=room.at[to, :, :, spot, :],
                dst_ref=landed.at[slot, :, :, spot, :],
                send_sem=field_sent.at[i],
                recv_sem=field_come.at[i],
                device_id=place(base + to),
                device_id_type=pl.DeviceIdType.MESH,
            )

        def field_mine(i):
            spot = pl.ds(pl.multiple_of(i * TILE, TILE), TILE)
            return pltpu.make_async_copy(
                room.at[slot, :, :, spot, :], landed.at[slot, :, :, spot, :], field_own.at[i]
            )

        @pl.when(step > 0)
        def _():
            def run(k, carry):
                field_move(tile, k).start()
                return carry

            lax.fori_loop(1, own, run, 0)
            field_mine(tile).start()

    @pl.when(step == pl.num_programs(0) - 1)
    def _():
        all_moves(lambda copy: copy.wait_send())
        if counted:

            def run(i, carry):
                spot = pl.ds(pl.multiple_of(i * TILE, TILE), TILE)
                gone = room.at[pl.ds(0, own - 1), :, :, spot, :]
                come = landed.at[pl.ds(0, own - 1), :, :, spot, :]
                pltpu.make_async_copy(gone, gone, field_sent.at[i]).wait()
                pltpu.make_async_copy(come, come, field_come.at[i]).wait()
                field_mine(i).wait()
                return carry

            lax.fori_loop(0, rows // TILE, run, 0)


def narrow_body(vorticity_grid, forcing_grid, cutoff, forcing_shells):
    rows, grid = vorticity_grid.shape
    total = lax.axis_size("gx") * lax.axis_size("gy")
    own = total // 2
    rank = lax.axis_index("gx") * lax.axis_size("gy") + lax.axis_index("gy")
    half, lane_rank = rank // own, rank % own
    halves = [list(range(own)), list(range(own, total))]
    tables = wave_tables(grid, total, rows)
    half_low = LOW // 2
    unit = 2.0 * math.pi / grid
    cuts = 2
    cut = rows // cuts

    def exchange(values, groups=None):
        return lax.all_to_all(
            values, AXES, split_axis=0, concat_axis=0, tiled=True, axis_index_groups=groups
        )

    first_row = jnp.where(half == 0, 0, grid // 2) + lane_rank * rows
    first_wave = rank * rows - jnp.where(half == 0, 0, grid)

    def forward_y(fields, table):
        first = contract("tda,abx->tdbx", tables["y1"], fields)
        return contract("tDcdb,tdbx->Dctx", table, first)

    slope_of = (
        rows * jnp.arange(own)[None, :] + jnp.arange(rows)[:, None] - half * (grid // 2)
    ).astype(jnp.float32) * unit
    slope_table = tables["iyd"] * slope_of[:, None, None, :, None]

    def inverse_y(waves, table):
        first = contract("tdbrc,rctx->tdbx", table, waves)
        return contract("atd,tdbx->abx", tables["iy1"], first)

    tw_cos = tables["tw"][0][:, None, :]
    tw_sin = tables["tw"][1][:, None, :]
    flip = jnp.where((half == 1) & (jnp.arange(total) % 2 == 1), -1.0, 1.0)[:, None, None]
    tw_cos_back, tw_sin_back = tw_cos * flip, tw_sin * flip

    def forward_x(waves):
        first = contract("pdsc,sctl->pdtl", tables["x1"], waves)
        real, imag = first[:, 0], first[:, 1]
        first = jnp.stack([real * tw_cos + imag * tw_sin, imag * tw_cos - real * tw_sin], 1)
        return contract("pctl,cldq->pdtq", first, tables["x2"])

    def inverse_x(waves):
        first = contract("pctq,cqdl->pdtl", waves, tables["ix2"])
        real, imag = first[:, 0], first[:, 1]
        first = jnp.stack(
            [real * tw_cos_back - imag * tw_sin_back, imag * tw_cos_back + real * tw_sin_back], 1
        )
        return contract("sdpc,pctl->sdtl", tables["ix1"], first)

    p_ids = jnp.arange(total, dtype=jnp.int32)[:, None, None]
    q_ids = jnp.arange(rows, dtype=jnp.int32)[None, None, :]
    kx_ids = p_ids + total * q_ids
    wave_x = jnp.where(kx_ids < grid // 2, kx_ids, kx_ids - grid)
    deriv_x = jnp.where(kx_ids == grid // 2, 0, wave_x).astype(jnp.float32) * unit
    origin = lane_rank == 0
    extra_wave = jnp.where(half == 0, -(grid // 2), 0) + jnp.zeros((1, 1, 1), jnp.int32)

    def wave_y_of(piece):
        return first_wave + cut * piece + jnp.arange(cut, dtype=jnp.int32)[None, :, None]

    def laplacian(rows_y):
        return (wave_x * wave_x + rows_y * rows_y).astype(jnp.float32) * (unit * unit)

    def inverse_laplacian(rows_y):
        squares = wave_x * wave_x + rows_y * rows_y
        lap = squares.astype(jnp.float32) * (unit * unit)
        return jnp.where(squares == 0, 0.0, 1.0 / jnp.maximum(lap, unit * unit))

    def dealias(rows_y):
        return (jnp.abs(wave_x) <= cutoff[0]) & (jnp.abs(rows_y) <= cutoff[0])

    def slope_x(pair):
        return (-deriv_x * pair[1], deriv_x * pair[0])

    def packed(main, extra, piece):
        real, imag = main
        if piece == 0:
            here = origin & (jnp.arange(cut) == 0)[None, :, None]
            real = jnp.where(here, real - extra[1], real)
            imag = jnp.where(here, imag + extra[0], imag)
        return jnp.stack([real, imag], 1)

    def spectra_of(sent):
        pieces, extra = [], None
        for piece in range(cuts):
            waves = exchange(sent[:, :, piece * cut : (piece + 1) * cut])
            if piece == 0:
                riding = waves[:, 1:, :1]
                extra = forward_x(jnp.concatenate([riding, jnp.zeros_like(riding)], 1))
                extra = (extra[:, 0], extra[:, 1])
                here = origin & (jnp.arange(cut) == 0)[:, None]
                clear = here & (jnp.arange(2) == 1)[:, None, None]
                waves = jnp.where(clear, 0.0, waves)
            out = forward_x(waves)
            pieces.append((out[:, 0], out[:, 1]))
        return pieces, extra

    def returned(pieces):
        return jnp.concatenate([exchange(inverse_x(part), halves) for part in pieces], 2)

    turned = vorticity_grid.T.reshape(rows, total, rows)
    start = forward_y(turned, tables["y2"])
    state, extra = spectra_of(start)

    share = half_low // total
    count_d = -(-half_low // rows)
    count_q = -(-half_low // total)
    force = forward_y(forcing_grid.T.reshape(rows, total, rows), tables["y2_low"][:, :count_d])
    force = force.transpose(0, 2, 1, 3).reshape(count_d * rows, 2, rows)[:half_low]
    force = exchange(force.reshape(total, share, 2, rows))
    force = forward_x(force.transpose(0, 2, 1, 3))
    force = jnp.concatenate([force[..., rows - count_q :], force[..., :count_q]], 3)
    force = force.transpose(2, 1, 3, 0).reshape(share, 2, LOW)
    force = lax.all_gather(force, AXES, axis=0, tiled=True)
    turned_force = jnp.roll(jnp.flip(force, 2), 1, 2) * jnp.array([1.0, -1.0])[None, :, None]
    turned_force = jnp.roll(jnp.flip(turned_force, 0), 1, 0)
    force_all = jnp.concatenate([turned_force, force], 0)

    def spread(part):
        part = part.reshape(part.shape[0], 2, 2 * count_q, total).transpose(1, 3, 0, 2)
        gap = jnp.zeros(part.shape[:3] + (rows - 2 * count_q,), jnp.float32)
        return jnp.concatenate([part[..., count_q:], gap, part[..., :count_q]], 3)

    def shell(rows_y):
        squares = wave_x * wave_x + rows_y * rows_y
        mask = jnp.zeros(squares.shape, bool)
        for index in range(SHELLS):
            radius = forcing_shells[index]
            mask = mask | ((radius * radius <= squares) & (squares < (radius + 1) * (radius + 1)))
        return mask

    def drive_of(piece):
        base = jnp.clip(first_wave + cut * piece + half_low, 0, LOW - cut)
        part = spread(lax.dynamic_slice_in_dim(force_all, base, cut, 0))
        mask = shell(wave_y_of(piece))
        return tuple(jnp.where(mask, part[c], 0.0) for c in (0, 1))

    drive = [drive_of(piece) for piece in range(cuts)]
    part = spread(force[:1])
    mask = shell(extra_wave)
    drive_extra = tuple(jnp.where(mask, part[c], 0.0) for c in (0, 1))

    waves_y = [wave_y_of(piece) for piece in range(cuts)]
    laps = [laplacian(rows_y) for rows_y in waves_y]
    inv_laps = [inverse_laplacian(rows_y) for rows_y in waves_y]
    masks = [dealias(rows_y) for rows_y in waves_y]
    lap_extra, inv_lap_extra = laplacian(extra_wave), inverse_laplacian(extra_wave)
    mask_extra = dealias(extra_wave)

    def fields_of(pieces, extra):
        psi_extra = tuple(inv_lap_extra * part for part in extra)
        psis = [tuple(inv * part for part in pair) for inv, pair in zip(inv_laps, pieces)]
        out = [
            [packed(psi, psi_extra, i) for i, psi in enumerate(psis)],
            [packed(slope_x(psi), slope_x(psi_extra), i) for i, psi in enumerate(psis)],
            [packed(slope_x(pair), slope_x(extra), i) for i, pair in enumerate(pieces)],
            [packed(pair, extra, i) for i, pair in enumerate(pieces)],
        ]
        return out

    def product(psi, psi_x, vort_x, vort):
        advect = inverse_y(psi, slope_table) * inverse_y(vort_x, tables["iy"])
        advect = advect - inverse_y(psi_x, tables["iy"]) * inverse_y(vort, slope_table)
        pieces, extra = spectra_of(forward_y(advect, tables["y2"]))
        terms = [
            tuple(d - jnp.where(mask, part, 0.0) for d, part in zip(ds, pair))
            for ds, mask, pair in zip(drive, masks, pieces)
        ]
        extra = tuple(d - jnp.where(mask_extra, part, 0.0) for d, part in zip(drive_extra, extra))
        return terms, extra

    own_start = lax.dynamic_slice_in_dim(start, half * own, own, 0)
    sent = fields_of(state, extra)[:3]
    first, first_extra = product(*[returned(part) for part in sent], own_start)

    def ahead_of(pair, lap, term):
        return tuple(
            part - time_step * viscosity * lap * part + time_step * add
            for part, add in zip(pair, term)
        )

    moved = [ahead_of(pair, lap, term) for pair, lap, term in zip(state, laps, first)]
    moved_extra = ahead_of(extra, lap_extra, first_extra)
    sent = fields_of(moved, moved_extra)
    second, _ = product(*[returned(part) for part in sent])

    def stepped(part, ahead, lap, one, two):
        return part + 0.5 * time_step * (one + two - viscosity * lap * (part + ahead))

    low_x = (wave_x >= -half_low) & (wave_x < half_low)
    outs, lows = [], []
    for i in range(cuts):
        low = low_x & (waves_y[i] >= -half_low) & (waves_y[i] < half_low)
        parts, low_parts = [], []
        for c in (0, 1):
            now = stepped(state[i][c], moved[i][c], laps[i], first[i][c], second[i][c])
            ahead = now + coarse_ratio * (now - state[i][c])
            parts.append(jnp.where(low, ahead, now))
            low_parts.append(
                jnp.concatenate([ahead[..., rows - count_q :], ahead[..., :count_q]], -1)
            )
        outs.append(jnp.stack(parts))
        lows.append(jnp.stack(low_parts))
    block = jnp.concatenate(lows, 2)
    spectrum = jnp.concatenate(outs, 2).transpose(0, 2, 3, 1).reshape(2, rows, grid)

    part_of = LOW // total
    signed = np.arange(LOW) - half_low
    spots = np.arange(LOW)
    col_cos, col_sin = (
        t.astype(np.float32) / 16.0 for t in turn(signed[:, None] * spots[None, :], LOW)
    )
    column = np.stack([np.stack([col_cos, col_sin]), np.stack([-col_sin, col_cos])])
    column = column.reshape(2, 2, 2 * count_q, total, LOW)
    mixed = contract("cptq,cdqpa->dta", block, column)
    mixed = mixed.reshape(2, rows, total, part_of).transpose(2, 0, 1, 3)
    mixed = exchange(mixed)
    mixed = jnp.concatenate([mixed[total - count_d :], mixed[:count_d]], 0)
    mixed = mixed.transpose(1, 0, 2, 3).reshape(2, 2 * count_d * rows, part_of)
    if count_d * rows != half_low:
        mixed = mixed[:, count_d * rows - half_low : count_d * rows + half_low]
    coarse = contract("cqa,cqb->ab", mixed, np.stack([col_cos, -col_sin]))
    return (spectrum, coarse)


def transfer_kernel(total, jobs, *refs):
    count = len(jobs)
    sources, results = refs[:count], refs[count : 2 * count]
    sent, arrived, local = refs[2 * count :]
    width = lax.axis_size("gy")
    me = lax.axis_index("gx") * width + lax.axis_index("gy")
    own = total // 2

    def copies(action):
        for index, (size, begin, extent, reach, mode) in enumerate(jobs):
            source, result = sources[index], results[index]
            base = (me // size) * size
            slot = me - base

            def block(place, rows):
                if mode == "gather":
                    return source
                if extent is None:
                    return source.at[place]
                return source.at[place, :, pl.ds(begin, rows), :]

            def landing(place, rows):
                if extent is None or rows == extent:
                    return result.at[place]
                return result.at[place, :, pl.ds(0, rows), :]

            def move(k, dest, rows):
                return pltpu.make_async_remote_copy(
                    src_ref=block(dest - base, rows),
                    dst_ref=landing(slot, rows),
                    send_sem=sent.at[index, k],
                    recv_sem=arrived.at[index, k],
                    device_id=(dest // width, dest % width),
                    device_id_type=pl.DeviceIdType.MESH,
                )

            def wanted(device):
                if reach is None:
                    return [(None, extent)]
                near = (device <= reach) | (device >= total - 1 - reach)
                out = [(near, extent)]
                if begin == 0:
                    out.append(((device == own) & (own > reach), TILE))
                return out

            def guarded(condition, run):
                if condition is None:
                    run()
                else:
                    pl.when(condition)(run)

            def one(k, carry):
                dest = base + (slot + k) % size
                if mode == "ends":
                    source_ok = (me < reach) | (me >= total - reach)
                    origin = (me - k + total) % total
                    origin_ok = (origin < reach) | (origin >= total - reach)
                    if action != "arrived":
                        guarded(source_ok, lambda: getattr(move(k, dest, extent), "start" if action == "start" else "wait_send")())
                    else:
                        guarded(origin_ok, lambda: move(k, dest, extent).wait_recv())
                    return carry
                for condition, rows in wanted(me if action == "arrived" else dest):
                    if action == "start":
                        guarded(condition, lambda: move(k, dest, rows).start())
                    elif action == "sent":
                        guarded(condition, lambda: move(k, dest, rows).wait_send())
                    else:
                        guarded(condition, lambda: move(k, dest, rows).wait_recv())
                return carry

            if action == "start":
                here = pltpu.make_async_copy(
                    block(slot, extent), landing(slot, extent), local.at[index]
                )
                here.start()
            lax.fori_loop(1, size, one, 0)
            if action == "arrived":
                pltpu.make_async_copy(
                    block(slot, extent), landing(slot, extent), local.at[index]
                ).wait()

    copies("start")
    copies("sent")
    copies("arrived")


def transfer(total, number, *jobs):
    shapes, plans = [], []
    for source, size, begin, extent, reach, mode in jobs:
        dims = source.shape
        if mode == "gather":
            dims = (size,) + dims
        elif extent is not None:
            dims = dims[:2] + (extent,) + dims[3:]
        shapes.append(jax.ShapeDtypeStruct(dims, source.dtype))
        plans.append((size, begin, extent, reach, mode))
    anywhere = pl.BlockSpec(memory_space=pl.ANY)
    widest = max(plan[0] for plan in plans)
    return pl.pallas_call(
        functools.partial(transfer_kernel, total, tuple(plans)),
        out_shape=shapes,
        in_specs=[anywhere] * len(plans),
        out_specs=[anywhere] * len(plans),
        scratch_shapes=[
            pltpu.SemaphoreType.DMA((len(plans), widest)),
            pltpu.SemaphoreType.DMA((len(plans), widest)),
            pltpu.SemaphoreType.DMA((len(plans),)),
        ],
        compiler_params=pltpu.CompilerParams(has_side_effects=True),
        name=f"transfer{number}",
    )(*[job[0] for job in jobs])


def low_table(grid):
    angles = np.arange(grid)[:, None] * np.arange(LOW // 2)[None, :]
    cos_t, sin_t = turn(angles, grid)
    return (np.concatenate([cos_t, -sin_t], 1) / grid).astype(np.float32)


def force_rows(waves, rank):
    total, _, _, rows = waves.shape
    kx = np.arange(LOW) - LOW // 2
    cos_l, sin_l = turn(np.arange(rows)[:, None] * kx[None, :], total * rows)
    cos_s, sin_s = turn(np.arange(total)[:, None] * kx[None, :], total)
    table = rotation(cos_l, -sin_l, (2, 0))
    waves = contract("scnl,cldk->sdnk", waves, table)
    real, imag = waves[:, 0], waves[:, 1]
    c, s = (t.astype(np.float32)[:, None, :] for t in (cos_s, sin_s))
    return jnp.stack([(real * c + imag * s).sum(0), (imag * c - real * s).sum(0)])


def body(vorticity_grid, forcing_grid, cutoff, forcing_shells):
    rows, grid = vorticity_grid.shape
    total = lax.axis_size("gx") * lax.axis_size("gy")
    own = total // 2
    rank = lax.axis_index("gx") * lax.axis_size("gy") + lax.axis_index("gy")
    half, lane_rank = rank // own, rank % own
    half_low = LOW // 2
    unit = 2.0 * math.pi / grid

    first_wave = rank * rows - half * grid
    extra_wave = -(1 - half) * (grid // 2)
    info = jnp.stack(
        [
            first_wave, extra_wave, (lane_rank == 0).astype(jnp.int32), half * (grid // 2),
            cutoff[0], rank,
        ]
    ).astype(jnp.int32)
    side = (1.0 - 2.0 * half.astype(jnp.float32)).reshape(1)
    y_forth, y_back = y_tables(grid, total, rows)
    x_forth, x_back, twist = x_tables(grid, total, rows)
    y_forth, y_back = halves_of(y_forth), halves_of(y_back)
    x_forth, x_back = halves_of(x_forth), halves_of(x_back)
    smem = pl.BlockSpec(memory_space=pltpu.SMEM)
    vmem = pl.BlockSpec(memory_space=pltpu.VMEM)
    f32 = jnp.float32

    def shape(*dims):
        return jax.ShapeDtypeStruct(dims, f32)

    def scratch(*dims):
        return pltpu.VMEM(dims, f32)

    between = scratch(total, 2, TILE, rows)
    waves_room = scratch(total, 2 * rows, rows)
    send_shape = shape(total, 2, rows, rows)

    turned = vorticity_grid.reshape(rows, rows, total).transpose(2, 1, 0)
    start = pl.pallas_call(
        functools.partial(start_kernel, total, rows),
        out_shape=send_shape,
        in_specs=[vmem] * 3,
        out_specs=vmem,
        scratch_shapes=[waves_room, between],
        compiler_params=params(),
        name="start",
    )(turned, *y_forth)

    def product(*flat):
        return pl.pallas_call(
            functools.partial(product_kernel, total, rows, unit),
            out_shape=send_shape,
            in_specs=[smem] + [vmem] * (4 + len(flat)),
            out_specs=vmem,
            scratch_shapes=[
                waves_room, scratch(total, rows, rows), scratch(total, rows, rows), between,
            ],
            compiler_params=params(),
            name="product",
        )(info, *y_forth, *y_back, *flat)

    def spectral(stage, source, *inputs):
        steps = rows // TILE + 1
        count = 3 + stage if stage < 2 else 0
        plain = pl.BlockSpec((total, 2, TILE, rows), lambda i: (0, 0, i, 0))
        main = pl.BlockSpec((total, 2, TILE, rows), lambda i: (0, 0, jnp.maximum(i - 1, 0), 0))
        anywhere = pl.BlockSpec(memory_space=pl.ANY)
        whole = shape(total, 2, rows + TILE, rows)
        fields = shape(own, count, 2, rows, rows)
        if stage < 2:
            outs, out_specs = [whole] * (1 + stage) + [fields], [plain] * (1 + stage) + [anywhere]
        else:
            outs, out_specs = [shape(total, 2, rows, rows)] * 2, [main] * 2
        tables = (twist, *x_forth, *x_back)
        rooms = [
            scratch(total * TILE, 2 * rows), scratch(total * TILE, 2 * rows), between,
            scratch(4, own, TILE, rows), scratch(total, 2, rows, rows),
            pltpu.SemaphoreType.DMA((rows // PART, total)),
            pltpu.SemaphoreType.DMA((rows // PART,)),
            pltpu.SemaphoreType.DMA((1,)),
        ]
        if count:
            rooms += [scratch(own, count, 2, rows, rows)]
            rooms += [pltpu.SemaphoreType.DMA((rows // TILE,))] * 3
        return pl.pallas_call(
            functools.partial(spectral_kernel, total, rows, grid, stage),
            grid=(steps,),
            out_shape=outs,
            in_specs=[smem, smem, anywhere] + [vmem] * len(tables) + [plain] * len(inputs),
            out_specs=out_specs,
            scratch_shapes=rooms,
            compiler_params=pltpu.CompilerParams(
                vmem_limit_bytes=56 * 1024 * 1024, has_side_effects=True
            ),
            name=f"spectral{stage}",
        )(info, side, source, *tables, *inputs)

    count_q = -(-half_low // total)
    share = half_low // total
    force = contract("xy,yn->nx", forcing_grid, low_table(grid))
    force = force.reshape(2, total, share, rows).transpose(1, 0, 2, 3)
    (force,) = transfer(total, 0, (force, total, 0, None, None, "all"))
    force = force_rows(force, rank)
    (force,) = transfer(total, 1, (force, total, 0, None, None, "gather"))
    force = force.transpose(0, 2, 1, 3).reshape(half_low, 2, LOW)
    turned_force = jnp.roll(jnp.flip(force, 2), 1, 2) * jnp.array([1.0, -1.0])[None, :, None]
    turned_force = jnp.roll(jnp.flip(turned_force, 0), 1, 0)
    force_all = jnp.concatenate([turned_force, force], 0)
    wave_kx = jnp.arange(LOW, dtype=jnp.int32)[None, None, :] - half_low

    def drive_rows(part, rows_y):
        squares = wave_kx * wave_kx + rows_y * rows_y
        mask = jnp.zeros(squares.shape, bool)
        for index in range(SHELLS):
            radius = forcing_shells[index]
            mask = mask | ((radius * radius <= squares) & (squares < (radius + 1) * (radius + 1)))
        return jnp.where(mask, part, 0.0)

    part = lax.dynamic_slice_in_dim(
        force_all, jnp.clip(first_wave + half_low, 0, LOW - rows), rows, 0
    )
    part = drive_rows(part, first_wave + jnp.arange(rows, dtype=jnp.int32)[:, None, None])
    extra = drive_rows(force[:1], extra_wave)
    extra = jnp.concatenate([extra, jnp.zeros((TILE - 1,) + extra.shape[1:], f32)], 0)
    part = jnp.concatenate([extra, part], 0)
    part = part.reshape(part.shape[0], 2, 2 * count_q, total).transpose(3, 1, 0, 2)
    gap = jnp.zeros(part.shape[:3] + (rows - 2 * count_q,), f32)
    drive = jnp.concatenate([part[..., count_q:], gap, part[..., :count_q]], 3)

    state, fields = spectral(0, start)
    own_start = lax.dynamic_slice_in_dim(start, half * own, own, 0)
    advect = product(fields, own_start)
    moved, first, fields = spectral(1, advect, state, drive)
    advect = product(fields)
    ahead, now = spectral(2, advect, state, moved, first, drive)
    block = jnp.concatenate([ahead[..., rows - count_q :], ahead[..., :count_q]], -1)
    spectrum = now.transpose(1, 2, 3, 0).reshape(2, rows, grid)

    part_of = LOW // total
    count_d = -(-half_low // rows)
    signed = np.arange(LOW) - half_low
    spots = np.arange(LOW)
    col_cos, col_sin = (
        t.astype(np.float32) / 16.0 for t in turn(signed[:, None] * spots[None, :], LOW)
    )
    column = np.stack([np.stack([col_cos, col_sin]), np.stack([-col_sin, col_cos])])
    column = column.reshape(2, 2, 2 * count_q, total, LOW)
    mixed = contract("pctq,cdqpa->adt", block, column).reshape(total, part_of, 2, rows)
    (mixed,) = transfer(total, 7, (mixed, total, 0, None, count_d, "ends"))
    mixed = jnp.concatenate([mixed[total - count_d :], mixed[:count_d]], 0)
    mixed = mixed.transpose(2, 0, 3, 1).reshape(2, 2 * count_d * rows, part_of)
    coarse = contract("cqa,cqb->ab", mixed, np.stack([col_cos, -col_sin]))
    return (spectrum, coarse)


def solution(mesh):
    placed = (P(AXES, None), P(AXES, None), P(), P())

    def run(vorticity_grid, *rest):
        rows = vorticity_grid.shape[0] // mesh.size
        chosen = body if rows % 128 == 0 and mesh.size >= 8 else narrow_body
        return jax.shard_map(
            chosen,
            mesh=mesh,
            in_specs=placed,
            out_specs=(P(None, AXES, None), P(AXES, None)),
            check_vma=False,
        )(vorticity_grid, *rest)

    return run
```

```python
import functools
import math

import jax
import jax.numpy as jnp
import numpy as np
from jax import lax
from jax.experimental import pallas as pl
from jax.experimental.pallas import tpu as pltpu
from jax.sharding import PartitionSpec as P

LOW = 256
SHELLS = 4
AXES = ("gx", "gy")

time_step = 0.05
viscosity = 0.05
coarse_ratio = 4.0


def contract(pattern, left_side, right_side):
    return jnp.einsum(pattern, left_side, right_side, precision=lax.Precision.HIGH)


def turn(product, length_of):
    phases = 2.0 * np.pi / length_of * (product % length_of)
    return np.cos(phases), np.sin(phases)


def rotation(cos_part, sin_part, axes):
    pairs = np.stack([np.stack([cos_part, -sin_part]), np.stack([sin_part, cos_part])])
    return np.moveaxis(pairs, (0, 1), axes).astype(np.float32)


def wave_tables(grid, total, rows):
    own = total // 2
    scale = 1.0 / math.sqrt(grid)
    t, a = np.arange(rows), np.arange(rows)
    b, D = np.arange(total), np.arange(total)
    out = {}
    cos_t, sin_t = turn(t[:, None] * a[None, :], rows)
    out["y1"] = np.stack([cos_t, -sin_t], 1).astype(np.float32)
    out["iy1"] = np.moveaxis(np.stack([cos_t, -sin_t], 1), 2, 0).astype(np.float32)
    ky = rows * D[None, :, None] + t[:, None, None]
    cos_t, sin_t = turn(ky * b[None, None, :], grid)
    sign = 1.0 - 2.0 * (b % 2)
    table = np.moveaxis(rotation(cos_t * scale, -sin_t * scale, (0, 1)), (0, 1), (2, 3))
    out["y2_low"] = table.copy()
    table[0, 0, 1] = np.stack([sign * scale, 0 * sign])
    table[0, own, 1] = np.stack([0 * sign + scale, 0 * sign])
    out["y2"] = table
    cos_t, sin_t = np.moveaxis(cos_t[:, :own], 1, 2), np.moveaxis(sin_t[:, :own], 1, 2)
    weight = np.where(ky[:, None, :own, 0] == 0, scale, 2.0 * scale)
    back = np.moveaxis(rotation(cos_t * weight, sin_t * weight, (0, 1)), (0, 1), (1, 4))
    back[0, :, :, 0, 1] = np.stack([sign * scale, 0 * sign])
    out["iy"] = back
    slope = np.moveaxis(rotation(-sin_t * weight, cos_t * weight, (0, 1)), (0, 1), (1, 4))
    slope[0, :, :, 0, :] = 0.0
    out["iyd"] = slope
    p, s = np.arange(total), np.arange(total)
    q, lane = np.arange(rows), np.arange(rows)
    cos_t, sin_t = turn(p[:, None] * s[None, :], total)
    out["x1"] = rotation(cos_t * scale, -sin_t * scale, (1, 3))
    cos_t, sin_t = turn(s[:own, None] * p[None, :], total)
    out["ix1"] = rotation(cos_t * scale, sin_t * scale, (1, 3))
    cos_t, sin_t = turn(q[:, None] * lane[None, :], rows)
    out["x2"] = rotation(cos_t.T, -sin_t.T, (2, 0))
    out["ix2"] = rotation(cos_t, sin_t, (2, 0))
    cos_t, sin_t = turn(p[:, None] * lane[None, :], grid)
    out["tw"] = np.stack([cos_t, sin_t]).astype(np.float32)
    return out


TILE = 16
PART = 32
GROUP = 4
FLIGHT = 2


def plus(one, two, sign=1.0):
    if two is None:
        return one
    if one is None:
        return tuple(sign * part for part in two)
    if sign > 0:
        return one[0] + two[0], one[1] + two[1]
    return one[0] - two[0], one[1] - two[1]


def turned_by(value, step, length, sign):
    if value is None:
        return None
    step = step % length
    real, imag = value
    if step == 0:
        return value
    if 2 * step == length:
        return -real, -imag
    if 4 * step == length:
        return (-imag, real) if sign > 0 else (imag, -real)
    if 4 * step == 3 * length:
        return (imag, -real) if sign > 0 else (-imag, real)
    angle = 2.0 * math.pi * step / length
    c, s = math.cos(angle), sign * math.sin(angle)
    return real * c - imag * s, real * s + imag * c


def small_fft(values, sign):
    size = len(values)
    if size == 1:
        return values
    even, odd = small_fft(values[::2], sign), small_fft(values[1::2], sign)
    odd = [turned_by(value, k, size, sign) for k, value in enumerate(odd)]
    return [plus(e, o) for e, o in zip(even, odd)] + [plus(e, o, -1.0) for e, o in zip(even, odd)]


def long_fft(total, load, store, between, sign, side=None):
    wide = 4
    deep = total // wide
    for j in range(deep):
        out = small_fft([load(deep * i + j) for i in range(wide)], sign)
        for u in range(wide):
            real, imag = turned_by(out[u], j * u, total, sign)
            between[u * deep + j, 0] = real
            between[u * deep + j, 1] = imag
    for u in range(wide):
        values = [(between[u * deep + j, 0], between[u * deep + j, 1]) for j in range(deep)]
        if side is None:
            for v, value in enumerate(small_fft(values, sign)):
                store(u + wide * v, value)
        else:
            even, odd = small_fft(values[::2], sign), small_fft(values[1::2], sign)
            for v in range(deep // 2):
                o = turned_by(odd[v], v, deep, sign)
                store(u + wide * v, (even[v][0] + side * o[0], even[v][1] + side * o[1]))


def split(value):
    high = value.astype(jnp.bfloat16)
    return high, (value - high.astype(jnp.float32)).astype(jnp.bfloat16)


def halves_of(table):
    table = np.asarray(table, np.float32)
    high = table.astype(jnp.bfloat16)
    return high, (table - high.astype(np.float32)).astype(jnp.bfloat16)


def dot(left, right):
    return jnp.dot(left, right, preferred_element_type=jnp.float32)


def stacked(table):
    return np.concatenate(halves_of(table), -2)


def table_times(table, data):
    rows, columns = table.shape[0] // 2, data.shape[1]
    found = dot(table, jnp.concatenate(split(data), 1))
    return found[:rows, :columns] + (found[:rows, columns:] + found[rows:, :columns])


def times_table(data, high_table, low_table):
    rows = data.shape[0]
    high, low = split(data)
    found = dot(jnp.concatenate([high, low], 0), high_table)
    return found[:rows] + (found[rows:] + dot(high, low_table))


def y_tables(grid, total, rows):
    scale = 1.0 / math.sqrt(grid)
    b, t, a = np.arange(total)[:, None, None], np.arange(rows)[None, :, None], np.arange(rows)
    cos_t, sin_t = turn(t * a * total + t * b, grid)
    forth = np.concatenate([cos_t, -sin_t], 1) * scale
    return forth, 2.0 * forth.transpose(0, 2, 1)


def x_tables(grid, total, rows):
    scale = 1.0 / math.sqrt(grid)
    l, q = np.arange(rows)[:, None], np.arange(rows)[None, :]
    cos_t, sin_t = turn(l * q, rows)
    forth = np.block([[cos_t, -sin_t], [sin_t, cos_t]]) * scale
    back = np.block([[cos_t, sin_t], [-sin_t, cos_t]]) * scale
    cos_t, sin_t = turn(np.arange(total)[:, None] * np.arange(rows)[None, :], grid)
    return forth, back, np.stack([cos_t, sin_t], 1).astype(np.float32)[:, :, None, :]


def params():
    return pltpu.CompilerParams(vmem_limit_bytes=56 * 1024 * 1024)


def forward_rows(total, rows, waves, out_ref, between):
    def tile(i, carry):
        spot = pl.ds(pl.multiple_of(i * TILE, TILE), TILE)
        low = pl.ds(pl.multiple_of(rows + i * TILE, TILE), TILE)

        def store(D, value):
            out_ref[D, 0, spot, :] = value[0]
            out_ref[D, 1, spot, :] = value[1]

        long_fft(total, lambda b: (waves[b, spot, :], waves[b, low, :]), store, between, -1.0)
        return carry

    lax.fori_loop(0, rows // TILE, tile, 0)
    top = pl.ds(0, 8)
    here = lax.broadcasted_iota(jnp.int32, (8, rows), 0) == 0
    middle = total // 2
    zero, other = out_ref[0, 0, top, :], out_ref[middle, 0, top, :]
    out_ref[0, 1, top, :] = jnp.where(here, other, out_ref[0, 1, top, :])
    out_ref[middle, 1, top, :] = jnp.where(here, zero, out_ref[middle, 1, top, :])


def start_kernel(total, rows, field, forth, out_ref, waves, between):
    def step(i, carry):
        spots = [i * GROUP + j for j in range(GROUP)]
        found = [table_times(forth[b], field[b]) for b in spots]
        for b, value in zip(spots, found):
            waves[b] = value
        return carry

    lax.fori_loop(0, total // GROUP, step, 0)
    forward_rows(total, rows, waves, out_ref, between)


def product_kernel(total, rows, unit, info, forth, back, *refs):
    fields, out_ref, waves, left, right, between = refs[0], *refs[-5:]
    psi, psi_x, vort_x = (fields.at[:, i] for i in range(3))
    own = total // 2
    vort = fields.at[:, 3] if len(refs) == 6 else refs[1].at[pl.ds(info[6], own)]
    own = total // 2
    offset = info[3]

    def waves_of(field, slope, begin):
        def tile(i, carry):
            spot = pl.ds(pl.multiple_of(i * TILE, TILE), TILE)
            top = pl.ds(pl.multiple_of(begin + i * TILE, TILE), TILE)
            low = pl.ds(pl.multiple_of(begin + rows + i * TILE, TILE), TILE)
            row = lax.broadcasted_iota(jnp.int32, (TILE, rows), 0) + (i * TILE + begin)
            here = row == 0

            def load(r):
                if r > own or (r == own and slope):
                    return None
                if r == own:
                    imag = field[0, 1, spot, :]
                    return jnp.where(here, 0.5 * imag, 0.0), jnp.zeros_like(imag)
                real, imag = field[r, 0, spot, :], field[r, 1, spot, :]
                if slope:
                    factor = (row + (r * rows - offset)).astype(jnp.float32) * unit
                    if r == 0:
                        factor = jnp.where(here, 0.0, factor)
                    return -factor * imag, factor * real
                if r == 0:
                    real = jnp.where(here, 0.5 * real, real)
                    imag = jnp.where(here, 0.0, imag)
                return real, imag

            def store(b, value):
                waves[b, top, :] = value[0]
                waves[b, low, :] = value[1]

            long_fft(total, load, store, between, 1.0)
            return carry

        lax.fori_loop(0, rows // TILE, tile, 0)

    def physical(spots):
        return [table_times(back[b], waves[b]) for b in spots]

    def each(step):
        def run(i, carry):
            step([i * GROUP + j for j in range(GROUP)])
            return carry

        lax.fori_loop(0, total // GROUP, run, 0)

    def put(ref, spots, values):
        for b, value in zip(spots, values):
            ref[b] = value

    def first(spots):
        put(left, spots, physical(spots))

    def second(spots):
        put(left, spots, [left[b] * value for b, value in zip(spots, physical(spots))])

    def third(spots):
        put(right, spots, physical(spots))

    def fourth(spots):
        values = physical(spots)
        advect = [left[b] - right[b] * value for b, value in zip(spots, values)]
        put(waves, spots, [table_times(forth[b], value) for b, value in zip(spots, advect)])

    for field, slope, step in (
        (psi, True, first), (vort_x, False, second), (psi_x, False, third), (vort, True, fourth),
    ):
        waves_of(field, slope, 0)
        each(step)
    forward_rows(total, rows, waves, out_ref, between)


def spectral_kernel(total, rows, grid, stage, *refs):
    refs = list(refs)

    def take(count):
        out = refs[:count]
        del refs[:count]
        return out

    info, side_of, source, twist, forth_hi, forth_lo, back_hi, back_lo = take(8)
    state_in = take(1)[0] if stage > 0 else None
    moved_in, first_in = take(2) if stage == 2 else (None, None)
    drive_in = take(1)[0] if stage > 0 else None
    state_out = take(1)[0] if stage == 0 else None
    moved_out, first_out = take(2) if stage == 1 else (None, None)
    ahead_out, now_out = take(2) if stage == 2 else (None, None)
    counted = 3 + stage if stage < 2 else 0
    landed = take(1)[0] if counted else None
    ins, outs, between, kept, arrived, sent_sem, come_sem, own_sem = take(8)
    room, field_sent, field_come, field_own = take(4) if counted else [None] * 4
    extra_first = True
    unit = 2.0 * math.pi / grid
    step = pl.program_id(0)
    riding = step == 0
    width = lax.axis_size("gy")
    me = lax.axis_index("gx") * width + lax.axis_index("gy")
    own = total // 2
    base = (me // own) * own
    slot = me - base
    reach = total if stage == 0 else (grid // 3) // rows
    parts = rows // PART

    def near(device):
        return (device <= reach) | (device >= total - 1 - reach)

    def place(device):
        return (device // width, device % width)

    def partner(k):
        return jnp.where(
            k % 2 == 0, (own - base) + (slot + k // 2) % own, base + (slot + (k + 1) // 2) % own
        )

    def move(part, k, extent):
        dest = partner(k)
        spot = pl.ds(pl.multiple_of(part * PART, PART), extent)
        return pltpu.make_async_remote_copy(
            src_ref=source.at[dest, :, spot, :],
            dst_ref=arrived.at[me, :, spot, :],
            send_sem=sent_sem.at[part, k],
            recv_sem=come_sem.at[part],
            device_id=place(dest),
            device_id_type=pl.DeviceIdType.MESH,
        )

    def all_moves(begin, end, act):
        def run(n, carry):
            part, k = n // (total - 1), n % (total - 1)
            dest = partner(k)

            @pl.when(near(dest))
            def _():
                act(move(part, k, PART))

            if reach < own:

                @pl.when((dest == own) & (part == 0))
                def _():
                    act(move(part, k, TILE))

            return carry

        lax.fori_loop(begin * (total - 1), end * (total - 1), run, 0)

    mine = pltpu.make_async_copy(source.at[me], arrived.at[me], own_sem.at[0])

    def await_part(part, extent):
        spot = pl.ds(pl.multiple_of(part * PART, PART), extent)
        ref = arrived.at[pl.ds(0, total - 1), :, spot, :]
        pltpu.make_async_copy(ref, ref, come_sem.at[part]).wait()

    @pl.when(riding)
    def _():
        all_moves(0, FLIGHT, lambda copy: copy.start())
        mine.start()
        mine.wait()

        if reach < own:

            @pl.when(me == own)
            def _():
                await_part(0, TILE)

    every = PART // TILE

    part_here = jnp.maximum(step - 1, 0) // every
    fresh = riding | ((step > 1) & ((step - 1) % every == 0))

    @pl.when(near(me) & fresh)
    def _():
        await_part(part_here, PART)

    @pl.when(fresh & (part_here < parts - FLIGHT))
    def _():
        all_moves(part_here + FLIGHT, part_here + FLIGHT + 1, lambda copy: copy.start())

    spot_in = pl.ds(pl.multiple_of(jnp.maximum(step - 1, 0) * TILE, TILE), TILE)
    origin = info[2] == 1
    tile = step - 1
    size = TILE
    shape = (size, rows)
    row = lax.broadcasted_iota(jnp.int32, shape, 0)
    first_here = (row == 0) & (tile == 0) & origin if extra_first else None
    side = side_of[0]

    def block(p):
        return pl.ds(pl.multiple_of(p * GROUP * size, GROUP * size), GROUP * size)

    def load(s):
        real, imag = arrived[s, 0, spot_in, :], arrived[s, 1, spot_in, :]
        if extra_first:
            ride = jnp.where(row == 0, imag, 0.0)
            imag = jnp.where(riding | first_here, 0.0, imag)
            real = jnp.where(riding, ride, real)
        return real, imag

    def store(p, value):
        c, s = twist[p, 0], twist[p, 1]
        ins[p * size : (p + 1) * size, :rows] = value[0] * c + value[1] * s
        ins[p * size : (p + 1) * size, rows:] = value[1] * c - value[0] * s

    long_fft(total, load, store, between, -1.0)
    chunk = 16 * size

    def multiply(hi, lo):
        def run(i, carry):
            spot = pl.ds(pl.multiple_of(i * chunk, chunk), chunk)
            outs[spot, :] = times_table(ins[spot, :], hi[...], lo[...])
            return carry

        lax.fori_loop(0, total * size // chunk, run, 0)

    multiply(forth_hi, forth_lo)
    wave_y = info[0] + tile * size + row
    if extra_first:
        wave_y = jnp.where(riding, info[1], wave_y)
    q = lax.broadcasted_iota(jnp.int32, shape, 1)
    cutoff = info[4]
    rows_kept = jnp.abs(wave_y) <= cutoff
    y_squared = wave_y * wave_y

    q = lax.broadcasted_iota(jnp.int32, (GROUP,) + shape, 2)
    lead = lax.broadcasted_iota(jnp.int32, (GROUP,) + shape, 0)
    wave_y, y_squared, rows_kept = wave_y[None], y_squared[None], rows_kept[None]

    def waves_x(p):
        kx = p * GROUP + lead + total * q
        wave = jnp.where(kx < grid // 2, kx, kx - grid)
        slope = jnp.where(kx == grid // 2, 0, wave).astype(jnp.float32) * unit
        return wave, slope

    def squares_of(wave):
        squares = wave * wave + y_squared
        return squares, squares.astype(jnp.float32) * (unit * unit)

    def spots(p):
        return pl.ds(p * GROUP, GROUP)

    def pair(ref, p):
        return ref[spots(p), 0], ref[spots(p), 1]

    def put(ref, p, value):
        ref[spots(p), 0] = value[0]
        ref[spots(p), 1] = value[1]

    step_size = time_step * viscosity

    def settle(p, carry):
        wave, _ = waves_x(p)
        squares, lap = squares_of(wave)
        found = tuple(
            part.reshape(GROUP, size, rows) for part in (outs[block(p), :rows], outs[block(p), rows:])
        )
        if stage == 0:
            put(state_out, p, found)
            return carry
        mask = rows_kept & (jnp.abs(wave) <= cutoff)
        term = tuple(d - jnp.where(mask, part, 0.0) for d, part in zip(pair(drive_in, p), found))
        state = pair(state_in, p)
        if stage == 1:
            put(first_out, p, term)
            put(moved_out, p, tuple(s - step_size * lap * s + time_step * t for s, t in zip(state, term)))
            return carry
        low = LOW // 2
        inside = (wave >= -low) & (wave < low) & (wave_y >= -low) & (wave_y < low)
        moved, first = pair(moved_in, p), pair(first_in, p)
        for c in (0, 1):
            linear = viscosity * lap * (state[c] + moved[c])
            now = state[c] + 0.5 * time_step * (first[c] + term[c] - linear)
            ahead = now + coarse_ratio * (now - state[c])
            ahead_out[spots(p), c] = pltpu.roll(ahead, LOW // 2 // total, 2)
            now_out[spots(p), c] = jnp.where(inside, ahead, now)
        return carry

    lax.fori_loop(0, total // GROUP, settle, 0)
    whole = state_out if stage == 0 else moved_out

    for index in range(counted):

        def fill(p, carry):
            wave, slope = waves_x(p)
            real, imag = pair(whole, p)
            if index < 2:
                squares, lap = squares_of(wave)
                inverse = jnp.where(squares == 0, 0.0, 1.0 / jnp.maximum(lap, unit * unit))
                real, imag = inverse * real, inverse * imag
            if index in (1, 2):
                real, imag = -slope * imag, slope * real
            ins[block(p), :rows] = real.reshape(GROUP * size, rows)
            ins[block(p), rows:] = imag.reshape(GROUP * size, rows)
            return carry

        lax.fori_loop(0, total // GROUP, fill, 0)
        multiply(back_hi, back_lo)

        def load_back(p):
            real, imag = outs[p * size : (p + 1) * size, :rows], outs[p * size : (p + 1) * size, rows:]
            c, s = twist[p, 0], twist[p, 1]
            return real * c - imag * s, imag * c + real * s

        def store_back(s, value):
            real, imag = value
            if extra_first:
                imag = jnp.where(first_here, kept[index, s], imag)
                kept[index, s] = real
            room[s, index, 0, spot_in, :] = real
            room[s, index, 1, spot_in, :] = imag

        long_fft(total, load_back, store_back, between, 1.0, side)

    if counted:

        def field_move(i, k):
            spot = pl.ds(pl.multiple_of(i * TILE, TILE), TILE)
            to = (slot + k) % own
            return pltpu.make_async_remote_copy(
                src_ref=room.at[to, :, :, spot, :],
                dst_ref=landed.at[slot, :, :, spot, :],
                send_sem=field_sent.at[i],
                recv_sem=field_come.at[i],
                device_id=place(base + to),
                device_id_type=pl.DeviceIdType.MESH,
            )

        def field_mine(i):
            spot = pl.ds(pl.multiple_of(i * TILE, TILE), TILE)
            return pltpu.make_async_copy(
                room.at[slot, :, :, spot, :], landed.at[slot, :, :, spot, :], field_own.at[i]
            )

        @pl.when(step > 0)
        def _():
            def run(k, carry):
                field_move(tile, k).start()
                return carry

            lax.fori_loop(1, own, run, 0)
            field_mine(tile).start()

    @pl.when(step == pl.num_programs(0) - 1)
    def _():
        all_moves(0, parts, lambda copy: copy.wait_send())
        if counted:

            def run(i, carry):
                spot = pl.ds(pl.multiple_of(i * TILE, TILE), TILE)
                gone = room.at[pl.ds(0, own - 1), :, :, spot, :]
                come = landed.at[pl.ds(0, own - 1), :, :, spot, :]
                pltpu.make_async_copy(gone, gone, field_sent.at[i]).wait()
                pltpu.make_async_copy(come, come, field_come.at[i]).wait()
                field_mine(i).wait()
                return carry

            lax.fori_loop(0, rows // TILE, run, 0)


def narrow_body(vorticity_grid, forcing_grid, cutoff, forcing_shells):
    rows, grid = vorticity_grid.shape
    total = lax.axis_size("gx") * lax.axis_size("gy")
    own = total // 2
    rank = lax.axis_index("gx") * lax.axis_size("gy") + lax.axis_index("gy")
    half, lane_rank = rank // own, rank % own
    halves = [list(range(own)), list(range(own, total))]
    tables = wave_tables(grid, total, rows)
    half_low = LOW // 2
    unit = 2.0 * math.pi / grid
    cuts = 2
    cut = rows // cuts

    def exchange(values, groups=None):
        return lax.all_to_all(
            values, AXES, split_axis=0, concat_axis=0, tiled=True, axis_index_groups=groups
        )

    first_row = jnp.where(half == 0, 0, grid // 2) + lane_rank * rows
    first_wave = rank * rows - jnp.where(half == 0, 0, grid)

    def forward_y(fields, table):
        first = contract("tda,abx->tdbx", tables["y1"], fields)
        return contract("tDcdb,tdbx->Dctx", table, first)

    slope_of = (
        rows * jnp.arange(own)[None, :] + jnp.arange(rows)[:, None] - half * (grid // 2)
    ).astype(jnp.float32) * unit
    slope_table = tables["iyd"] * slope_of[:, None, None, :, None]

    def inverse_y(waves, table):
        first = contract("tdbrc,rctx->tdbx", table, waves)
        return contract("atd,tdbx->abx", tables["iy1"], first)

    tw_cos = tables["tw"][0][:, None, :]
    tw_sin = tables["tw"][1][:, None, :]
    flip = jnp.where((half == 1) & (jnp.arange(total) % 2 == 1), -1.0, 1.0)[:, None, None]
    tw_cos_back, tw_sin_back = tw_cos * flip, tw_sin * flip

    def forward_x(waves):
        first = contract("pdsc,sctl->pdtl", tables["x1"], waves)
        real, imag = first[:, 0], first[:, 1]
        first = jnp.stack([real * tw_cos + imag * tw_sin, imag * tw_cos - real * tw_sin], 1)
        return contract("pctl,cldq->pdtq", first, tables["x2"])

    def inverse_x(waves):
        first = contract("pctq,cqdl->pdtl", waves, tables["ix2"])
        real, imag = first[:, 0], first[:, 1]
        first = jnp.stack(
            [real * tw_cos_back - imag * tw_sin_back, imag * tw_cos_back + real * tw_sin_back], 1
        )
        return contract("sdpc,pctl->sdtl", tables["ix1"], first)

    p_ids = jnp.arange(total, dtype=jnp.int32)[:, None, None]
    q_ids = jnp.arange(rows, dtype=jnp.int32)[None, None, :]
    kx_ids = p_ids + total * q_ids
    wave_x = jnp.where(kx_ids < grid // 2, kx_ids, kx_ids - grid)
    deriv_x = jnp.where(kx_ids == grid // 2, 0, wave_x).astype(jnp.float32) * unit
    origin = lane_rank == 0
    extra_wave = jnp.where(half == 0, -(grid // 2), 0) + jnp.zeros((1, 1, 1), jnp.int32)

    def wave_y_of(piece):
        return first_wave + cut * piece + jnp.arange(cut, dtype=jnp.int32)[None, :, None]

    def laplacian(rows_y):
        return (wave_x * wave_x + rows_y * rows_y).astype(jnp.float32) * (unit * unit)

    def inverse_laplacian(rows_y):
        squares = wave_x * wave_x + rows_y * rows_y
        lap = squares.astype(jnp.float32) * (unit * unit)
        return jnp.where(squares == 0, 0.0, 1.0 / jnp.maximum(lap, unit * unit))

    def dealias(rows_y):
        return (jnp.abs(wave_x) <= cutoff[0]) & (jnp.abs(rows_y) <= cutoff[0])

    def slope_x(pair):
        return (-deriv_x * pair[1], deriv_x * pair[0])

    def packed(main, extra, piece):
        real, imag = main
        if piece == 0:
            here = origin & (jnp.arange(cut) == 0)[None, :, None]
            real = jnp.where(here, real - extra[1], real)
            imag = jnp.where(here, imag + extra[0], imag)
        return jnp.stack([real, imag], 1)

    def spectra_of(sent):
        pieces, extra = [], None
        for piece in range(cuts):
            waves = exchange(sent[:, :, piece * cut : (piece + 1) * cut])
            if piece == 0:
                riding = waves[:, 1:, :1]
                extra = forward_x(jnp.concatenate([riding, jnp.zeros_like(riding)], 1))
                extra = (extra[:, 0], extra[:, 1])
                here = origin & (jnp.arange(cut) == 0)[:, None]
                clear = here & (jnp.arange(2) == 1)[:, None, None]
                waves = jnp.where(clear, 0.0, waves)
            out = forward_x(waves)
            pieces.append((out[:, 0], out[:, 1]))
        return pieces, extra

    def returned(pieces):
        return jnp.concatenate([exchange(inverse_x(part), halves) for part in pieces], 2)

    turned = vorticity_grid.T.reshape(rows, total, rows)
    start = forward_y(turned, tables["y2"])
    state, extra = spectra_of(start)

    share = half_low // total
    count_d = -(-half_low // rows)
    count_q = -(-half_low // total)
    force = forward_y(forcing_grid.T.reshape(rows, total, rows), tables["y2_low"][:, :count_d])
    force = force.transpose(0, 2, 1, 3).reshape(count_d * rows, 2, rows)[:half_low]
    force = exchange(force.reshape(total, share, 2, rows))
    force = forward_x(force.transpose(0, 2, 1, 3))
    force = jnp.concatenate([force[..., rows - count_q :], force[..., :count_q]], 3)
    force = force.transpose(2, 1, 3, 0).reshape(share, 2, LOW)
    force = lax.all_gather(force, AXES, axis=0, tiled=True)
    turned_force = jnp.roll(jnp.flip(force, 2), 1, 2) * jnp.array([1.0, -1.0])[None, :, None]
    turned_force = jnp.roll(jnp.flip(turned_force, 0), 1, 0)
    force_all = jnp.concatenate([turned_force, force], 0)

    def spread(part):
        part = part.reshape(part.shape[0], 2, 2 * count_q, total).transpose(1, 3, 0, 2)
        gap = jnp.zeros(part.shape[:3] + (rows - 2 * count_q,), jnp.float32)
        return jnp.concatenate([part[..., count_q:], gap, part[..., :count_q]], 3)

    def shell(rows_y):
        squares = wave_x * wave_x + rows_y * rows_y
        mask = jnp.zeros(squares.shape, bool)
        for index in range(SHELLS):
            radius = forcing_shells[index]
            mask = mask | ((radius * radius <= squares) & (squares < (radius + 1) * (radius + 1)))
        return mask

    def drive_of(piece):
        base = jnp.clip(first_wave + cut * piece + half_low, 0, LOW - cut)
        part = spread(lax.dynamic_slice_in_dim(force_all, base, cut, 0))
        mask = shell(wave_y_of(piece))
        return tuple(jnp.where(mask, part[c], 0.0) for c in (0, 1))

    drive = [drive_of(piece) for piece in range(cuts)]
    part = spread(force[:1])
    mask = shell(extra_wave)
    drive_extra = tuple(jnp.where(mask, part[c], 0.0) for c in (0, 1))

    waves_y = [wave_y_of(piece) for piece in range(cuts)]
    laps = [laplacian(rows_y) for rows_y in waves_y]
    inv_laps = [inverse_laplacian(rows_y) for rows_y in waves_y]
    masks = [dealias(rows_y) for rows_y in waves_y]
    lap_extra, inv_lap_extra = laplacian(extra_wave), inverse_laplacian(extra_wave)
    mask_extra = dealias(extra_wave)

    def fields_of(pieces, extra):
        psi_extra = tuple(inv_lap_extra * part for part in extra)
        psis = [tuple(inv * part for part in pair) for inv, pair in zip(inv_laps, pieces)]
        out = [
            [packed(psi, psi_extra, i) for i, psi in enumerate(psis)],
            [packed(slope_x(psi), slope_x(psi_extra), i) for i, psi in enumerate(psis)],
            [packed(slope_x(pair), slope_x(extra), i) for i, pair in enumerate(pieces)],
            [packed(pair, extra, i) for i, pair in enumerate(pieces)],
        ]
        return out

    def product(psi, psi_x, vort_x, vort):
        advect = inverse_y(psi, slope_table) * inverse_y(vort_x, tables["iy"])
        advect = advect - inverse_y(psi_x, tables["iy"]) * inverse_y(vort, slope_table)
        pieces, extra = spectra_of(forward_y(advect, tables["y2"]))
        terms = [
            tuple(d - jnp.where(mask, part, 0.0) for d, part in zip(ds, pair))
            for ds, mask, pair in zip(drive, masks, pieces)
        ]
        extra = tuple(d - jnp.where(mask_extra, part, 0.0) for d, part in zip(drive_extra, extra))
        return terms, extra

    own_start = lax.dynamic_slice_in_dim(start, half * own, own, 0)
    sent = fields_of(state, extra)[:3]
    first, first_extra = product(*[returned(part) for part in sent], own_start)

    def ahead_of(pair, lap, term):
        return tuple(
            part - time_step * viscosity * lap * part + time_step * add
            for part, add in zip(pair, term)
        )

    moved = [ahead_of(pair, lap, term) for pair, lap, term in zip(state, laps, first)]
    moved_extra = ahead_of(extra, lap_extra, first_extra)
    sent = fields_of(moved, moved_extra)
    second, _ = product(*[returned(part) for part in sent])

    def stepped(part, ahead, lap, one, two):
        return part + 0.5 * time_step * (one + two - viscosity * lap * (part + ahead))

    low_x = (wave_x >= -half_low) & (wave_x < half_low)
    outs, lows = [], []
    for i in range(cuts):
        low = low_x & (waves_y[i] >= -half_low) & (waves_y[i] < half_low)
        parts, low_parts = [], []
        for c in (0, 1):
            now = stepped(state[i][c], moved[i][c], laps[i], first[i][c], second[i][c])
            ahead = now + coarse_ratio * (now - state[i][c])
            parts.append(jnp.where(low, ahead, now))
            low_parts.append(
                jnp.concatenate([ahead[..., rows - count_q :], ahead[..., :count_q]], -1)
            )
        outs.append(jnp.stack(parts))
        lows.append(jnp.stack(low_parts))
    block = jnp.concatenate(lows, 2)
    spectrum = jnp.concatenate(outs, 2).transpose(0, 2, 3, 1).reshape(2, rows, grid)

    part_of = LOW // total
    signed = np.arange(LOW) - half_low
    spots = np.arange(LOW)
    col_cos, col_sin = (
        t.astype(np.float32) / 16.0 for t in turn(signed[:, None] * spots[None, :], LOW)
    )
    column = np.stack([np.stack([col_cos, col_sin]), np.stack([-col_sin, col_cos])])
    column = column.reshape(2, 2, 2 * count_q, total, LOW)
    mixed = contract("cptq,cdqpa->dta", block, column)
    mixed = mixed.reshape(2, rows, total, part_of).transpose(2, 0, 1, 3)
    mixed = exchange(mixed)
    mixed = jnp.concatenate([mixed[total - count_d :], mixed[:count_d]], 0)
    mixed = mixed.transpose(1, 0, 2, 3).reshape(2, 2 * count_d * rows, part_of)
    if count_d * rows != half_low:
        mixed = mixed[:, count_d * rows - half_low : count_d * rows + half_low]
    coarse = contract("cqa,cqb->ab", mixed, np.stack([col_cos, -col_sin]))
    return (spectrum, coarse)


def low_spectrum(grid_part, rank, total):
    rows, grid = grid_part.shape
    low = LOW // 2
    cos_t, sin_t = turn(np.arange(grid)[:, None] * np.arange(low)[None, :], grid)
    table = (np.concatenate([cos_t, -sin_t], 1) / grid).astype(np.float32)
    waves = contract("xy,yn->xn", grid_part, table)
    waves = jnp.stack([waves[:, :low], waves[:, low:]])
    x = rank * rows + jnp.arange(rows, dtype=jnp.int32)
    kx = jnp.arange(LOW, dtype=jnp.int32) - low
    angle = ((kx[None, :] * x[:, None]) & (grid - 1)).astype(jnp.float32) * (2.0 * math.pi / grid)
    c, s = jnp.cos(angle), jnp.sin(angle)
    turns = jnp.stack([jnp.stack([c, -s]), jnp.stack([s, c])])
    found = contract("cxn,cdxk->ndk", waves, turns)
    return lax.psum(found, AXES)


def body(vorticity_grid, forcing_grid, cutoff, forcing_shells):
    rows, grid = vorticity_grid.shape
    total = lax.axis_size("gx") * lax.axis_size("gy")
    own = total // 2
    rank = lax.axis_index("gx") * lax.axis_size("gy") + lax.axis_index("gy")
    half, lane_rank = rank // own, rank % own
    half_low = LOW // 2
    unit = 2.0 * math.pi / grid

    first_wave = rank * rows - half * grid
    extra_wave = -(1 - half) * (grid // 2)
    info = jnp.stack(
        [
            first_wave, extra_wave, (lane_rank == 0).astype(jnp.int32), half * (grid // 2),
            cutoff[0], rank, half * own,
        ]
    ).astype(jnp.int32)
    side = (1.0 - 2.0 * half.astype(jnp.float32)).reshape(1)
    y_forth, y_back = y_tables(grid, total, rows)
    x_forth, x_back, twist = x_tables(grid, total, rows)
    y_forth, y_back = stacked(y_forth), stacked(y_back)
    x_forth, x_back = halves_of(x_forth), halves_of(x_back)
    smem = pl.BlockSpec(memory_space=pltpu.SMEM)
    vmem = pl.BlockSpec(memory_space=pltpu.VMEM)
    f32 = jnp.float32

    def shape(*dims):
        return jax.ShapeDtypeStruct(dims, f32)

    def scratch(*dims):
        return pltpu.VMEM(dims, f32)

    between = scratch(total, 2, TILE, rows)
    waves_room = scratch(total, 2 * rows, rows)
    send_shape = shape(total, 2, rows, rows)

    turned = vorticity_grid.reshape(rows, rows, total).transpose(2, 1, 0)
    start = pl.pallas_call(
        functools.partial(start_kernel, total, rows),
        out_shape=send_shape,
        in_specs=[vmem] * 2,
        out_specs=vmem,
        scratch_shapes=[waves_room, between],
        compiler_params=params(),
        name="start",
    )(turned, y_forth)

    def product(*flat):
        return pl.pallas_call(
            functools.partial(product_kernel, total, rows, unit),
            out_shape=send_shape,
            in_specs=[smem] + [vmem] * (2 + len(flat)),
            out_specs=vmem,
            scratch_shapes=[
                waves_room, scratch(total, rows, rows), scratch(total, rows, rows), between,
            ],
            compiler_params=params(),
            cost_estimate=pl.CostEstimate(flops=10**10, bytes_accessed=0, transcendentals=0),
            name="product",
        )(info, y_forth, y_back, *flat)

    def spectral(stage, source, *inputs):
        steps = rows // TILE + 1
        count = 3 + stage if stage < 2 else 0
        plain = pl.BlockSpec((total, 2, TILE, rows), lambda i: (0, 0, i, 0))
        main = pl.BlockSpec((total, 2, TILE, rows), lambda i: (0, 0, jnp.maximum(i - 1, 0), 0))
        anywhere = pl.BlockSpec(memory_space=pl.ANY)
        whole = shape(total, 2, rows + TILE, rows)
        fields = shape(own, count, 2, rows, rows)
        if stage < 2:
            outs, out_specs = [whole] * (1 + stage) + [fields], [plain] * (1 + stage) + [anywhere]
        else:
            outs, out_specs = [shape(total, 2, rows, rows)] * 2, [main] * 2
        tables = (twist, *x_forth, *x_back)
        rooms = [
            scratch(total * TILE, 2 * rows), scratch(total * TILE, 2 * rows), between,
            scratch(4, own, TILE, rows), scratch(total, 2, rows, rows),
            pltpu.SemaphoreType.DMA((rows // PART, total)),
            pltpu.SemaphoreType.DMA((rows // PART,)),
            pltpu.SemaphoreType.DMA((1,)),
        ]
        if count:
            rooms += [scratch(own, count, 2, rows, rows)]
            rooms += [pltpu.SemaphoreType.DMA((rows // TILE,))] * 3
        return pl.pallas_call(
            functools.partial(spectral_kernel, total, rows, grid, stage),
            grid=(steps,),
            out_shape=outs,
            in_specs=[smem, smem, anywhere] + [vmem] * len(tables) + [plain] * len(inputs),
            out_specs=out_specs,
            scratch_shapes=rooms,
            compiler_params=pltpu.CompilerParams(
                vmem_limit_bytes=56 * 1024 * 1024, has_side_effects=True
            ),
            cost_estimate=pl.CostEstimate(flops=10**10, bytes_accessed=0, transcendentals=0),
            name=f"spectral{stage}",
        )(info, side, source, *tables, *inputs)

    count_q = -(-half_low // total)
    force = low_spectrum(forcing_grid, rank, total)
    turned_force = jnp.roll(jnp.flip(force, 2), 1, 2) * jnp.array([1.0, -1.0])[None, :, None]
    turned_force = jnp.roll(jnp.flip(turned_force, 0), 1, 0)
    force_all = jnp.concatenate([turned_force, force], 0)
    wave_kx = jnp.arange(LOW, dtype=jnp.int32)[None, None, :] - half_low

    def drive_rows(part, rows_y):
        squares = wave_kx * wave_kx + rows_y * rows_y
        mask = jnp.zeros(squares.shape, bool)
        for index in range(SHELLS):
            radius = forcing_shells[index]
            mask = mask | ((radius * radius <= squares) & (squares < (radius + 1) * (radius + 1)))
        return jnp.where(mask, part, 0.0)

    part = lax.dynamic_slice_in_dim(
        force_all, jnp.clip(first_wave + half_low, 0, LOW - rows), rows, 0
    )
    part = drive_rows(part, first_wave + jnp.arange(rows, dtype=jnp.int32)[:, None, None])
    extra = drive_rows(force[:1], extra_wave)
    extra = jnp.concatenate([extra, jnp.zeros((TILE - 1,) + extra.shape[1:], f32)], 0)
    part = jnp.concatenate([extra, part], 0)
    part = part.reshape(part.shape[0], 2, 2 * count_q, total).transpose(3, 1, 0, 2)
    gap = jnp.zeros(part.shape[:3] + (rows - 2 * count_q,), f32)
    drive = jnp.concatenate([part[..., count_q:], gap, part[..., :count_q]], 3)

    state, fields = spectral(0, start)
    advect = product(fields, start)
    moved, first, fields = spectral(1, advect, state, drive)
    advect = product(fields)
    ahead, now = spectral(2, advect, state, moved, first, drive)
    block = ahead[..., : 2 * count_q]
    spectrum = now.transpose(1, 2, 3, 0).reshape(2, rows, grid)

    part_of = LOW // total
    count_d = -(-half_low // rows)
    signed = np.arange(LOW) - half_low
    spots = np.arange(LOW)
    col_cos, col_sin = (
        t.astype(np.float32) / 16.0 for t in turn(signed[:, None] * spots[None, :], LOW)
    )
    column = np.stack([np.stack([col_cos, col_sin]), np.stack([-col_sin, col_cos])])
    column = column.reshape(2, 2, 2 * count_q, total, LOW)
    mixed = contract("pctq,cdqpa->adt", block, column).reshape(total, part_of, 2, rows)
    mixed = lax.all_to_all(mixed, AXES, split_axis=0, concat_axis=0, tiled=True)
    mixed = jnp.concatenate([mixed[total - count_d :], mixed[:count_d]], 0)
    mixed = mixed.transpose(2, 0, 3, 1).reshape(2, 2 * count_d * rows, part_of)
    coarse = contract("cqa,cqb->ab", mixed, np.stack([col_cos, -col_sin]))
    return (spectrum, coarse)


def solution(mesh):
    placed = (P(AXES, None), P(AXES, None), P(), P())

    def run(vorticity_grid, *rest):
        rows = vorticity_grid.shape[0] // mesh.size
        chosen = body if rows % 128 == 0 and mesh.size >= 8 else narrow_body
        return jax.shard_map(
            chosen,
            mesh=mesh,
            in_specs=placed,
            out_specs=(P(None, AXES, None), P(AXES, None)),
            check_vma=False,
        )(vorticity_grid, *rest)

    return run
```

```python
import functools
import math

import jax
import jax.numpy as jnp
import numpy as np
from jax import lax
from jax.experimental import pallas as pl
from jax.experimental.pallas import tpu as pltpu
from jax.sharding import PartitionSpec as P

LOW = 256
SHELLS = 4
AXES = ("gx", "gy")

time_step = 0.05
viscosity = 0.05
coarse_ratio = 4.0


def contract(pattern, left_side, right_side):
    return jnp.einsum(pattern, left_side, right_side, precision=lax.Precision.HIGH)


def turn(product, length_of):
    phases = 2.0 * np.pi / length_of * (product % length_of)
    return np.cos(phases), np.sin(phases)


def rotation(cos_part, sin_part, axes):
    pairs = np.stack([np.stack([cos_part, -sin_part]), np.stack([sin_part, cos_part])])
    return np.moveaxis(pairs, (0, 1), axes).astype(np.float32)


def wave_tables(grid, total, rows):
    own = total // 2
    scale = 1.0 / math.sqrt(grid)
    t, a = np.arange(rows), np.arange(rows)
    b, D = np.arange(total), np.arange(total)
    out = {}
    cos_t, sin_t = turn(t[:, None] * a[None, :], rows)
    out["y1"] = np.stack([cos_t, -sin_t], 1).astype(np.float32)
    out["iy1"] = np.moveaxis(np.stack([cos_t, -sin_t], 1), 2, 0).astype(np.float32)
    ky = rows * D[None, :, None] + t[:, None, None]
    cos_t, sin_t = turn(ky * b[None, None, :], grid)
    sign = 1.0 - 2.0 * (b % 2)
    table = np.moveaxis(rotation(cos_t * scale, -sin_t * scale, (0, 1)), (0, 1), (2, 3))
    out["y2_low"] = table.copy()
    table[0, 0, 1] = np.stack([sign * scale, 0 * sign])
    table[0, own, 1] = np.stack([0 * sign + scale, 0 * sign])
    out["y2"] = table
    cos_t, sin_t = np.moveaxis(cos_t[:, :own], 1, 2), np.moveaxis(sin_t[:, :own], 1, 2)
    weight = np.where(ky[:, None, :own, 0] == 0, scale, 2.0 * scale)
    back = np.moveaxis(rotation(cos_t * weight, sin_t * weight, (0, 1)), (0, 1), (1, 4))
    back[0, :, :, 0, 1] = np.stack([sign * scale, 0 * sign])
    out["iy"] = back
    slope = np.moveaxis(rotation(-sin_t * weight, cos_t * weight, (0, 1)), (0, 1), (1, 4))
    slope[0, :, :, 0, :] = 0.0
    out["iyd"] = slope
    p, s = np.arange(total), np.arange(total)
    q, lane = np.arange(rows), np.arange(rows)
    cos_t, sin_t = turn(p[:, None] * s[None, :], total)
    out["x1"] = rotation(cos_t * scale, -sin_t * scale, (1, 3))
    cos_t, sin_t = turn(s[:own, None] * p[None, :], total)
    out["ix1"] = rotation(cos_t * scale, sin_t * scale, (1, 3))
    cos_t, sin_t = turn(q[:, None] * lane[None, :], rows)
    out["x2"] = rotation(cos_t.T, -sin_t.T, (2, 0))
    out["ix2"] = rotation(cos_t, sin_t, (2, 0))
    cos_t, sin_t = turn(p[:, None] * lane[None, :], grid)
    out["tw"] = np.stack([cos_t, sin_t]).astype(np.float32)
    return out


TILE = 16
PART = 32
GROUP = 4
FLIGHT = 4


def plus(one, two, sign=1.0):
    if two is None:
        return one
    if one is None:
        return tuple(sign * part for part in two)
    if sign > 0:
        return one[0] + two[0], one[1] + two[1]
    return one[0] - two[0], one[1] - two[1]


def turned_by(value, step, length, sign):
    if value is None:
        return None
    step = step % length
    real, imag = value
    if step == 0:
        return value
    if 2 * step == length:
        return -real, -imag
    if 4 * step == length:
        return (-imag, real) if sign > 0 else (imag, -real)
    if 4 * step == 3 * length:
        return (imag, -real) if sign > 0 else (-imag, real)
    angle = 2.0 * math.pi * step / length
    c, s = math.cos(angle), sign * math.sin(angle)
    return real * c - imag * s, real * s + imag * c


def small_fft(values, sign):
    size = len(values)
    if size == 1:
        return values
    even, odd = small_fft(values[::2], sign), small_fft(values[1::2], sign)
    odd = [turned_by(value, k, size, sign) for k, value in enumerate(odd)]
    return [plus(e, o) for e, o in zip(even, odd)] + [plus(e, o, -1.0) for e, o in zip(even, odd)]


def long_fft(total, load, store, between, sign, side=None):
    wide = 4
    deep = total // wide
    for j in range(deep):
        out = small_fft([load(deep * i + j) for i in range(wide)], sign)
        for u in range(wide):
            real, imag = turned_by(out[u], j * u, total, sign)
            between[u * deep + j, 0] = real
            between[u * deep + j, 1] = imag
    for u in range(wide):
        values = [(between[u * deep + j, 0], between[u * deep + j, 1]) for j in range(deep)]
        if side is None:
            for v, value in enumerate(small_fft(values, sign)):
                store(u + wide * v, value)
        else:
            even, odd = small_fft(values[::2], sign), small_fft(values[1::2], sign)
            for v in range(deep // 2):
                o = turned_by(odd[v], v, deep, sign)
                store(u + wide * v, (even[v][0] + side * o[0], even[v][1] + side * o[1]))


def split(value):
    high = value.astype(jnp.bfloat16)
    return high, (value - high.astype(jnp.float32)).astype(jnp.bfloat16)


def halves_of(table):
    table = np.asarray(table, np.float32)
    high = table.astype(jnp.bfloat16)
    return high, (table - high.astype(np.float32)).astype(jnp.bfloat16)


def dot(left, right):
    return jnp.dot(left, right, preferred_element_type=jnp.float32)


def stacked(table):
    return np.concatenate(halves_of(table), -2)


def table_times(table, data):
    rows, columns = table.shape[0] // 2, data.shape[1]
    found = dot(table, jnp.concatenate(split(data), 1))
    return found[:rows, :columns] + (found[:rows, columns:] + found[rows:, :columns])


def times_table(data, high_table, low_table):
    rows = data.shape[0]
    high, low = split(data)
    found = dot(jnp.concatenate([high, low], 0), high_table)
    return found[:rows] + (found[rows:] + dot(high, low_table))


def y_tables(grid, total, rows):
    scale = 1.0 / math.sqrt(grid)
    b, t, a = np.arange(total)[:, None, None], np.arange(rows)[None, :, None], np.arange(rows)
    cos_t, sin_t = turn(t * a * total + t * b, grid)
    forth = np.concatenate([cos_t, -sin_t], 1) * scale
    return forth, 2.0 * forth.transpose(0, 2, 1)


def x_tables(grid, total, rows):
    scale = 1.0 / math.sqrt(grid)
    l, q = np.arange(rows)[:, None], np.arange(rows)[None, :]
    cos_t, sin_t = turn(l * q, rows)
    forth = np.block([[cos_t, -sin_t], [sin_t, cos_t]]) * scale
    back = np.block([[cos_t, sin_t], [-sin_t, cos_t]]) * scale
    cos_t, sin_t = turn(np.arange(total)[:, None] * np.arange(rows)[None, :], grid)
    return forth, back, np.stack([cos_t, sin_t], 1).astype(np.float32)[:, :, None, :]


def params():
    return pltpu.CompilerParams(vmem_limit_bytes=56 * 1024 * 1024)


def forward_rows(total, rows, waves, out_ref, between):
    def tile(i, carry):
        spot = pl.ds(pl.multiple_of(i * TILE, TILE), TILE)
        low = pl.ds(pl.multiple_of(rows + i * TILE, TILE), TILE)

        def store(D, value):
            out_ref[D, 0, spot, :] = value[0]
            out_ref[D, 1, spot, :] = value[1]

        long_fft(total, lambda b: (waves[b, spot, :], waves[b, low, :]), store, between, -1.0)
        return carry

    lax.fori_loop(0, rows // TILE, tile, 0)
    top = pl.ds(0, 8)
    here = lax.broadcasted_iota(jnp.int32, (8, rows), 0) == 0
    middle = total // 2
    zero, other = out_ref[0, 0, top, :], out_ref[middle, 0, top, :]
    out_ref[0, 1, top, :] = jnp.where(here, other, out_ref[0, 1, top, :])
    out_ref[middle, 1, top, :] = jnp.where(here, zero, out_ref[middle, 1, top, :])


def start_kernel(total, rows, field, forth, out_ref, waves, between):
    def step(i, carry):
        spots = [i * GROUP + j for j in range(GROUP)]
        found = [table_times(forth[b], field[b]) for b in spots]
        for b, value in zip(spots, found):
            waves[b] = value
        return carry

    lax.fori_loop(0, total // GROUP, step, 0)
    forward_rows(total, rows, waves, out_ref, between)


def product_kernel(total, rows, unit, info, forth, back, *refs):
    fields, out_ref, waves, left, right, between = refs[0], *refs[-5:]
    psi, psi_x, vort_x = (fields.at[:, i] for i in range(3))
    own = total // 2
    vort = fields.at[:, 3] if len(refs) == 6 else refs[1].at[pl.ds(info[6], own)]
    own = total // 2
    offset = info[3]

    def waves_of(field, slope, begin):
        def tile(i, carry):
            spot = pl.ds(pl.multiple_of(i * TILE, TILE), TILE)
            top = pl.ds(pl.multiple_of(begin + i * TILE, TILE), TILE)
            low = pl.ds(pl.multiple_of(begin + rows + i * TILE, TILE), TILE)
            row = lax.broadcasted_iota(jnp.int32, (TILE, rows), 0) + (i * TILE + begin)
            here = row == 0

            def load(r):
                if r > own or (r == own and slope):
                    return None
                if r == own:
                    imag = field[0, 1, spot, :]
                    return jnp.where(here, 0.5 * imag, 0.0), jnp.zeros_like(imag)
                real, imag = field[r, 0, spot, :], field[r, 1, spot, :]
                if slope:
                    factor = (row + (r * rows - offset)).astype(jnp.float32) * unit
                    if r == 0:
                        factor = jnp.where(here, 0.0, factor)
                    return -factor * imag, factor * real
                if r == 0:
                    real = jnp.where(here, 0.5 * real, real)
                    imag = jnp.where(here, 0.0, imag)
                return real, imag

            def store(b, value):
                waves[b, top, :] = value[0]
                waves[b, low, :] = value[1]

            long_fft(total, load, store, between, 1.0)
            return carry

        lax.fori_loop(0, rows // TILE, tile, 0)

    def physical(spots):
        return [table_times(back[b], waves[b]) for b in spots]

    def each(step):
        def run(i, carry):
            step([i * GROUP + j for j in range(GROUP)])
            return carry

        lax.fori_loop(0, total // GROUP, run, 0)

    def put(ref, spots, values):
        for b, value in zip(spots, values):
            ref[b] = value

    def first(spots):
        put(left, spots, physical(spots))

    def second(spots):
        put(left, spots, [left[b] * value for b, value in zip(spots, physical(spots))])

    def third(spots):
        put(right, spots, physical(spots))

    def fourth(spots):
        values = physical(spots)
        advect = [left[b] - right[b] * value for b, value in zip(spots, values)]
        put(waves, spots, [table_times(forth[b], value) for b, value in zip(spots, advect)])

    for field, slope, step in (
        (psi, True, first), (vort_x, False, second), (psi_x, False, third), (vort, True, fourth),
    ):
        waves_of(field, slope, 0)
        each(step)
    forward_rows(total, rows, waves, out_ref, between)


def spectral_kernel(total, rows, grid, stage, *refs):
    refs = list(refs)

    def take(count):
        out = refs[:count]
        del refs[:count]
        return out

    info, side_of, source, twist, forth_hi, forth_lo, back_hi, back_lo = take(8)
    state_in = take(1)[0] if stage > 0 else None
    moved_in, first_in = take(2) if stage == 2 else (None, None)
    drive_in = take(1)[0] if stage > 0 else None
    state_out = take(1)[0] if stage == 0 else None
    moved_out, first_out = take(2) if stage == 1 else (None, None)
    ahead_out, now_out = take(2) if stage == 2 else (None, None)
    counted = 3 + stage if stage < 2 else 0
    landed = take(1)[0] if counted else None
    ins, outs, between, kept, arrived, sent_sem, come_sem, own_sem = take(8)
    room, field_sent, field_come, field_own = take(4) if counted else [None] * 4
    extra_first = True
    unit = 2.0 * math.pi / grid
    step = pl.program_id(0)
    riding = step == 0
    width = lax.axis_size("gy")
    me = lax.axis_index("gx") * width + lax.axis_index("gy")
    own = total // 2
    base = (me // own) * own
    slot = me - base
    reach = total if stage == 0 else (grid // 3) // rows
    parts = rows // PART

    def near(device):
        return (device <= reach) | (device >= total - 1 - reach)

    def place(device):
        return (device // width, device % width)

    def partner(k):
        return jnp.where(
            k % 2 == 0, (own - base) + (slot + k // 2) % own, base + (slot + (k + 1) // 2) % own
        )

    def move(part, k, extent):
        dest = partner(k)
        spot = pl.ds(pl.multiple_of(part * PART, PART), extent)
        return pltpu.make_async_remote_copy(
            src_ref=source.at[dest, :, spot, :],
            dst_ref=arrived.at[me, :, spot, :],
            send_sem=sent_sem.at[part, k],
            recv_sem=come_sem.at[part],
            device_id=place(dest),
            device_id_type=pl.DeviceIdType.MESH,
        )

    def all_moves(begin, end, act):
        def run(n, carry):
            part, k = n // (total - 1), n % (total - 1)
            dest = partner(k)

            @pl.when(near(dest))
            def _():
                act(move(part, k, PART))

            if reach < own:

                @pl.when((dest == own) & (part == 0))
                def _():
                    act(move(part, k, TILE))

            return carry

        lax.fori_loop(begin * (total - 1), end * (total - 1), run, 0)

    mine = pltpu.make_async_copy(source.at[me], arrived.at[me], own_sem.at[0])

    def await_part(part, extent):
        spot = pl.ds(pl.multiple_of(part * PART, PART), extent)
        ref = arrived.at[pl.ds(0, total - 1), :, spot, :]
        pltpu.make_async_copy(ref, ref, come_sem.at[part]).wait()

    @pl.when(riding)
    def _():
        all_moves(0, FLIGHT, lambda copy: copy.start())
        mine.start()
        mine.wait()

        if reach < own:

            @pl.when(me == own)
            def _():
                await_part(0, TILE)

    every = PART // TILE

    part_here = jnp.maximum(step - 1, 0) // every
    fresh = riding | ((step > 1) & ((step - 1) % every == 0))

    @pl.when(near(me) & fresh)
    def _():
        await_part(part_here, PART)

    @pl.when(fresh & (part_here < parts - FLIGHT))
    def _():
        all_moves(part_here + FLIGHT, part_here + FLIGHT + 1, lambda copy: copy.start())

    spot_in = pl.ds(pl.multiple_of(jnp.maximum(step - 1, 0) * TILE, TILE), TILE)
    origin = info[2] == 1
    tile = step - 1
    size = TILE
    shape = (size, rows)
    row = lax.broadcasted_iota(jnp.int32, shape, 0)
    first_here = (row == 0) & (tile == 0) & origin if extra_first else None
    side = side_of[0]

    def block(p):
        return pl.ds(pl.multiple_of(p * GROUP * size, GROUP * size), GROUP * size)

    def load(s):
        real, imag = arrived[s, 0, spot_in, :], arrived[s, 1, spot_in, :]
        if extra_first:
            ride = jnp.where(row == 0, imag, 0.0)
            imag = jnp.where(riding | first_here, 0.0, imag)
            real = jnp.where(riding, ride, real)
        return real, imag

    def store(p, value):
        c, s = twist[p, 0], twist[p, 1]
        ins[p * size : (p + 1) * size, :rows] = value[0] * c + value[1] * s
        ins[p * size : (p + 1) * size, rows:] = value[1] * c - value[0] * s

    long_fft(total, load, store, between, -1.0)
    chunk = 16 * size

    def multiply(hi, lo):
        def run(i, carry):
            spot = pl.ds(pl.multiple_of(i * chunk, chunk), chunk)
            outs[spot, :] = times_table(ins[spot, :], hi[...], lo[...])
            return carry

        lax.fori_loop(0, total * size // chunk, run, 0)

    multiply(forth_hi, forth_lo)
    wave_y = info[0] + tile * size + row
    if extra_first:
        wave_y = jnp.where(riding, info[1], wave_y)
    q = lax.broadcasted_iota(jnp.int32, shape, 1)
    cutoff = info[4]
    rows_kept = jnp.abs(wave_y) <= cutoff
    y_squared = wave_y * wave_y

    q = lax.broadcasted_iota(jnp.int32, (GROUP,) + shape, 2)
    lead = lax.broadcasted_iota(jnp.int32, (GROUP,) + shape, 0)
    wave_y, y_squared, rows_kept = wave_y[None], y_squared[None], rows_kept[None]

    def waves_x(p):
        kx = p * GROUP + lead + total * q
        wave = jnp.where(kx < grid // 2, kx, kx - grid)
        slope = jnp.where(kx == grid // 2, 0, wave).astype(jnp.float32) * unit
        return wave, slope

    def squares_of(wave):
        squares = wave * wave + y_squared
        return squares, squares.astype(jnp.float32) * (unit * unit)

    def spots(p):
        return pl.ds(p * GROUP, GROUP)

    def pair(ref, p):
        return ref[spots(p), 0], ref[spots(p), 1]

    def put(ref, p, value):
        ref[spots(p), 0] = value[0]
        ref[spots(p), 1] = value[1]

    step_size = time_step * viscosity

    def settle(p, carry):
        wave, _ = waves_x(p)
        squares, lap = squares_of(wave)
        found = tuple(
            part.reshape(GROUP, size, rows) for part in (outs[block(p), :rows], outs[block(p), rows:])
        )
        if stage == 0:
            put(state_out, p, found)
            return carry
        mask = rows_kept & (jnp.abs(wave) <= cutoff)
        term = tuple(d - jnp.where(mask, part, 0.0) for d, part in zip(pair(drive_in, p), found))
        state = pair(state_in, p)
        if stage == 1:
            put(first_out, p, term)
            put(moved_out, p, tuple(s - step_size * lap * s + time_step * t for s, t in zip(state, term)))
            return carry
        low = LOW // 2
        inside = (wave >= -low) & (wave < low) & (wave_y >= -low) & (wave_y < low)
        moved, first = pair(moved_in, p), pair(first_in, p)
        for c in (0, 1):
            linear = viscosity * lap * (state[c] + moved[c])
            now = state[c] + 0.5 * time_step * (first[c] + term[c] - linear)
            ahead = now + coarse_ratio * (now - state[c])
            ahead_out[spots(p), c] = pltpu.roll(ahead, LOW // 2 // total, 2)
            now_out[spots(p), c] = jnp.where(inside, ahead, now)
        return carry

    lax.fori_loop(0, total // GROUP, settle, 0)
    whole = state_out if stage == 0 else moved_out

    for index in range(counted):

        def fill(p, carry):
            wave, slope = waves_x(p)
            real, imag = pair(whole, p)
            if index < 2:
                squares, lap = squares_of(wave)
                inverse = jnp.where(squares == 0, 0.0, 1.0 / jnp.maximum(lap, unit * unit))
                real, imag = inverse * real, inverse * imag
            if index in (1, 2):
                real, imag = -slope * imag, slope * real
            ins[block(p), :rows] = real.reshape(GROUP * size, rows)
            ins[block(p), rows:] = imag.reshape(GROUP * size, rows)
            return carry

        lax.fori_loop(0, total // GROUP, fill, 0)
        multiply(back_hi, back_lo)

        def load_back(p):
            real, imag = outs[p * size : (p + 1) * size, :rows], outs[p * size : (p + 1) * size, rows:]
            c, s = twist[p, 0], twist[p, 1]
            return real * c - imag * s, imag * c + real * s

        def store_back(s, value):
            real, imag = value
            if extra_first:
                imag = jnp.where(first_here, kept[index, s], imag)
                kept[index, s] = real
            room[s, index, 0, spot_in, :] = real
            room[s, index, 1, spot_in, :] = imag

        long_fft(total, load_back, store_back, between, 1.0, side)

    if counted:

        def field_move(i, k):
            spot = pl.ds(pl.multiple_of(i * TILE, TILE), TILE)
            to = (slot + k) % own
            return pltpu.make_async_remote_copy(
                src_ref=room.at[to, :, :, spot, :],
                dst_ref=landed.at[slot, :, :, spot, :],
                send_sem=field_sent.at[i],
                recv_sem=field_come.at[i],
                device_id=place(base + to),
                device_id_type=pl.DeviceIdType.MESH,
            )

        def field_mine(i):
            spot = pl.ds(pl.multiple_of(i * TILE, TILE), TILE)
            return pltpu.make_async_copy(
                room.at[slot, :, :, spot, :], landed.at[slot, :, :, spot, :], field_own.at[i]
            )

        @pl.when(step > 0)
        def _():
            def run(k, carry):
                field_move(tile, k).start()
                return carry

            lax.fori_loop(1, own, run, 0)
            field_mine(tile).start()

    @pl.when(step == pl.num_programs(0) - 1)
    def _():
        all_moves(0, parts, lambda copy: copy.wait_send())
        if counted:

            def run(i, carry):
                spot = pl.ds(pl.multiple_of(i * TILE, TILE), TILE)
                gone = room.at[pl.ds(0, own - 1), :, :, spot, :]
                come = landed.at[pl.ds(0, own - 1), :, :, spot, :]
                pltpu.make_async_copy(gone, gone, field_sent.at[i]).wait()
                pltpu.make_async_copy(come, come, field_come.at[i]).wait()
                field_mine(i).wait()
                return carry

            lax.fori_loop(0, rows // TILE, run, 0)


def narrow_body(vorticity_grid, forcing_grid, cutoff, forcing_shells):
    rows, grid = vorticity_grid.shape
    total = lax.axis_size("gx") * lax.axis_size("gy")
    own = total // 2
    rank = lax.axis_index("gx") * lax.axis_size("gy") + lax.axis_index("gy")
    half, lane_rank = rank // own, rank % own
    halves = [list(range(own)), list(range(own, total))]
    tables = wave_tables(grid, total, rows)
    half_low = LOW // 2
    unit = 2.0 * math.pi / grid
    cuts = 2
    cut = rows // cuts

    def exchange(values, groups=None):
        return lax.all_to_all(
            values, AXES, split_axis=0, concat_axis=0, tiled=True, axis_index_groups=groups
        )

    first_row = jnp.where(half == 0, 0, grid // 2) + lane_rank * rows
    first_wave = rank * rows - jnp.where(half == 0, 0, grid)

    def forward_y(fields, table):
        first = contract("tda,abx->tdbx", tables["y1"], fields)
        return contract("tDcdb,tdbx->Dctx", table, first)

    slope_of = (
        rows * jnp.arange(own)[None, :] + jnp.arange(rows)[:, None] - half * (grid // 2)
    ).astype(jnp.float32) * unit
    slope_table = tables["iyd"] * slope_of[:, None, None, :, None]

    def inverse_y(waves, table):
        first = contract("tdbrc,rctx->tdbx", table, waves)
        return contract("atd,tdbx->abx", tables["iy1"], first)

    tw_cos = tables["tw"][0][:, None, :]
    tw_sin = tables["tw"][1][:, None, :]
    flip = jnp.where((half == 1) & (jnp.arange(total) % 2 == 1), -1.0, 1.0)[:, None, None]
    tw_cos_back, tw_sin_back = tw_cos * flip, tw_sin * flip

    def forward_x(waves):
        first = contract("pdsc,sctl->pdtl", tables["x1"], waves)
        real, imag = first[:, 0], first[:, 1]
        first = jnp.stack([real * tw_cos + imag * tw_sin, imag * tw_cos - real * tw_sin], 1)
        return contract("pctl,cldq->pdtq", first, tables["x2"])

    def inverse_x(waves):
        first = contract("pctq,cqdl->pdtl", waves, tables["ix2"])
        real, imag = first[:, 0], first[:, 1]
        first = jnp.stack(
            [real * tw_cos_back - imag * tw_sin_back, imag * tw_cos_back + real * tw_sin_back], 1
        )
        return contract("sdpc,pctl->sdtl", tables["ix1"], first)

    p_ids = jnp.arange(total, dtype=jnp.int32)[:, None, None]
    q_ids = jnp.arange(rows, dtype=jnp.int32)[None, None, :]
    kx_ids = p_ids + total * q_ids
    wave_x = jnp.where(kx_ids < grid // 2, kx_ids, kx_ids - grid)
    deriv_x = jnp.where(kx_ids == grid // 2, 0, wave_x).astype(jnp.float32) * unit
    origin = lane_rank == 0
    extra_wave = jnp.where(half == 0, -(grid // 2), 0) + jnp.zeros((1, 1, 1), jnp.int32)

    def wave_y_of(piece):
        return first_wave + cut * piece + jnp.arange(cut, dtype=jnp.int32)[None, :, None]

    def laplacian(rows_y):
        return (wave_x * wave_x + rows_y * rows_y).astype(jnp.float32) * (unit * unit)

    def inverse_laplacian(rows_y):
        squares = wave_x * wave_x + rows_y * rows_y
        lap = squares.astype(jnp.float32) * (unit * unit)
        return jnp.where(squares == 0, 0.0, 1.0 / jnp.maximum(lap, unit * unit))

    def dealias(rows_y):
        return (jnp.abs(wave_x) <= cutoff[0]) & (jnp.abs(rows_y) <= cutoff[0])

    def slope_x(pair):
        return (-deriv_x * pair[1], deriv_x * pair[0])

    def packed(main, extra, piece):
        real, imag = main
        if piece == 0:
            here = origin & (jnp.arange(cut) == 0)[None, :, None]
            real = jnp.where(here, real - extra[1], real)
            imag = jnp.where(here, imag + extra[0], imag)
        return jnp.stack([real, imag], 1)

    def spectra_of(sent):
        pieces, extra = [], None
        for piece in range(cuts):
            waves = exchange(sent[:, :, piece * cut : (piece + 1) * cut])
            if piece == 0:
                riding = waves[:, 1:, :1]
                extra = forward_x(jnp.concatenate([riding, jnp.zeros_like(riding)], 1))
                extra = (extra[:, 0], extra[:, 1])
                here = origin & (jnp.arange(cut) == 0)[:, None]
                clear = here & (jnp.arange(2) == 1)[:, None, None]
                waves = jnp.where(clear, 0.0, waves)
            out = forward_x(waves)
            pieces.append((out[:, 0], out[:, 1]))
        return pieces, extra

    def returned(pieces):
        return jnp.concatenate([exchange(inverse_x(part), halves) for part in pieces], 2)

    turned = vorticity_grid.T.reshape(rows, total, rows)
    start = forward_y(turned, tables["y2"])
    state, extra = spectra_of(start)

    share = half_low // total
    count_d = -(-half_low // rows)
    count_q = -(-half_low // total)
    force = forward_y(forcing_grid.T.reshape(rows, total, rows), tables["y2_low"][:, :count_d])
    force = force.transpose(0, 2, 1, 3).reshape(count_d * rows, 2, rows)[:half_low]
    force = exchange(force.reshape(total, share, 2, rows))
    force = forward_x(force.transpose(0, 2, 1, 3))
    force = jnp.concatenate([force[..., rows - count_q :], force[..., :count_q]], 3)
    force = force.transpose(2, 1, 3, 0).reshape(share, 2, LOW)
    force = lax.all_gather(force, AXES, axis=0, tiled=True)
    turned_force = jnp.roll(jnp.flip(force, 2), 1, 2) * jnp.array([1.0, -1.0])[None, :, None]
    turned_force = jnp.roll(jnp.flip(turned_force, 0), 1, 0)
    force_all = jnp.concatenate([turned_force, force], 0)

    def spread(part):
        part = part.reshape(part.shape[0], 2, 2 * count_q, total).transpose(1, 3, 0, 2)
        gap = jnp.zeros(part.shape[:3] + (rows - 2 * count_q,), jnp.float32)
        return jnp.concatenate([part[..., count_q:], gap, part[..., :count_q]], 3)

    def shell(rows_y):
        squares = wave_x * wave_x + rows_y * rows_y
        mask = jnp.zeros(squares.shape, bool)
        for index in range(SHELLS):
            radius = forcing_shells[index]
            mask = mask | ((radius * radius <= squares) & (squares < (radius + 1) * (radius + 1)))
        return mask

    def drive_of(piece):
        base = jnp.clip(first_wave + cut * piece + half_low, 0, LOW - cut)
        part = spread(lax.dynamic_slice_in_dim(force_all, base, cut, 0))
        mask = shell(wave_y_of(piece))
        return tuple(jnp.where(mask, part[c], 0.0) for c in (0, 1))

    drive = [drive_of(piece) for piece in range(cuts)]
    part = spread(force[:1])
    mask = shell(extra_wave)
    drive_extra = tuple(jnp.where(mask, part[c], 0.0) for c in (0, 1))

    waves_y = [wave_y_of(piece) for piece in range(cuts)]
    laps = [laplacian(rows_y) for rows_y in waves_y]
    inv_laps = [inverse_laplacian(rows_y) for rows_y in waves_y]
    masks = [dealias(rows_y) for rows_y in waves_y]
    lap_extra, inv_lap_extra = laplacian(extra_wave), inverse_laplacian(extra_wave)
    mask_extra = dealias(extra_wave)

    def fields_of(pieces, extra):
        psi_extra = tuple(inv_lap_extra * part for part in extra)
        psis = [tuple(inv * part for part in pair) for inv, pair in zip(inv_laps, pieces)]
        out = [
            [packed(psi, psi_extra, i) for i, psi in enumerate(psis)],
            [packed(slope_x(psi), slope_x(psi_extra), i) for i, psi in enumerate(psis)],
            [packed(slope_x(pair), slope_x(extra), i) for i, pair in enumerate(pieces)],
            [packed(pair, extra, i) for i, pair in enumerate(pieces)],
        ]
        return out

    def product(psi, psi_x, vort_x, vort):
        advect = inverse_y(psi, slope_table) * inverse_y(vort_x, tables["iy"])
        advect = advect - inverse_y(psi_x, tables["iy"]) * inverse_y(vort, slope_table)
        pieces, extra = spectra_of(forward_y(advect, tables["y2"]))
        terms = [
            tuple(d - jnp.where(mask, part, 0.0) for d, part in zip(ds, pair))
            for ds, mask, pair in zip(drive, masks, pieces)
        ]
        extra = tuple(d - jnp.where(mask_extra, part, 0.0) for d, part in zip(drive_extra, extra))
        return terms, extra

    own_start = lax.dynamic_slice_in_dim(start, half * own, own, 0)
    sent = fields_of(state, extra)[:3]
    first, first_extra = product(*[returned(part) for part in sent], own_start)

    def ahead_of(pair, lap, term):
        return tuple(
            part - time_step * viscosity * lap * part + time_step * add
            for part, add in zip(pair, term)
        )

    moved = [ahead_of(pair, lap, term) for pair, lap, term in zip(state, laps, first)]
    moved_extra = ahead_of(extra, lap_extra, first_extra)
    sent = fields_of(moved, moved_extra)
    second, _ = product(*[returned(part) for part in sent])

    def stepped(part, ahead, lap, one, two):
        return part + 0.5 * time_step * (one + two - viscosity * lap * (part + ahead))

    low_x = (wave_x >= -half_low) & (wave_x < half_low)
    outs, lows = [], []
    for i in range(cuts):
        low = low_x & (waves_y[i] >= -half_low) & (waves_y[i] < half_low)
        parts, low_parts = [], []
        for c in (0, 1):
            now = stepped(state[i][c], moved[i][c], laps[i], first[i][c], second[i][c])
            ahead = now + coarse_ratio * (now - state[i][c])
            parts.append(jnp.where(low, ahead, now))
            low_parts.append(
                jnp.concatenate([ahead[..., rows - count_q :], ahead[..., :count_q]], -1)
            )
        outs.append(jnp.stack(parts))
        lows.append(jnp.stack(low_parts))
    block = jnp.concatenate(lows, 2)
    spectrum = jnp.concatenate(outs, 2).transpose(0, 2, 3, 1).reshape(2, rows, grid)

    part_of = LOW // total
    signed = np.arange(LOW) - half_low
    spots = np.arange(LOW)
    col_cos, col_sin = (
        t.astype(np.float32) / 16.0 for t in turn(signed[:, None] * spots[None, :], LOW)
    )
    column = np.stack([np.stack([col_cos, col_sin]), np.stack([-col_sin, col_cos])])
    column = column.reshape(2, 2, 2 * count_q, total, LOW)
    mixed = contract("cptq,cdqpa->dta", block, column)
    mixed = mixed.reshape(2, rows, total, part_of).transpose(2, 0, 1, 3)
    mixed = exchange(mixed)
    mixed = jnp.concatenate([mixed[total - count_d :], mixed[:count_d]], 0)
    mixed = mixed.transpose(1, 0, 2, 3).reshape(2, 2 * count_d * rows, part_of)
    if count_d * rows != half_low:
        mixed = mixed[:, count_d * rows - half_low : count_d * rows + half_low]
    coarse = contract("cqa,cqb->ab", mixed, np.stack([col_cos, -col_sin]))
    return (spectrum, coarse)


def low_spectrum(grid_part, rank, total):
    rows, grid = grid_part.shape
    low = LOW // 2
    cos_t, sin_t = turn(np.arange(grid)[:, None] * np.arange(low)[None, :], grid)
    table = (np.concatenate([cos_t, -sin_t], 1) / grid).astype(np.float32)
    waves = contract("xy,yn->xn", grid_part, table)
    waves = jnp.stack([waves[:, :low], waves[:, low:]])
    x = rank * rows + jnp.arange(rows, dtype=jnp.int32)
    kx = jnp.arange(LOW, dtype=jnp.int32) - low
    angle = ((kx[None, :] * x[:, None]) & (grid - 1)).astype(jnp.float32) * (2.0 * math.pi / grid)
    c, s = jnp.cos(angle), jnp.sin(angle)
    turns = jnp.stack([jnp.stack([c, -s]), jnp.stack([s, c])])
    found = contract("cxn,cdxk->ndk", waves, turns)
    return lax.psum(found, AXES)


def body(vorticity_grid, forcing_grid, cutoff, forcing_shells):
    rows, grid = vorticity_grid.shape
    total = lax.axis_size("gx") * lax.axis_size("gy")
    own = total // 2
    rank = lax.axis_index("gx") * lax.axis_size("gy") + lax.axis_index("gy")
    half, lane_rank = rank // own, rank % own
    half_low = LOW // 2
    unit = 2.0 * math.pi / grid

    first_wave = rank * rows - half * grid
    extra_wave = -(1 - half) * (grid // 2)
    info = jnp.stack(
        [
            first_wave, extra_wave, (lane_rank == 0).astype(jnp.int32), half * (grid // 2),
            cutoff[0], rank, half * own,
        ]
    ).astype(jnp.int32)
    side = (1.0 - 2.0 * half.astype(jnp.float32)).reshape(1)
    y_forth, y_back = y_tables(grid, total, rows)
    x_forth, x_back, twist = x_tables(grid, total, rows)
    y_forth, y_back = stacked(y_forth), stacked(y_back)
    x_forth, x_back = halves_of(x_forth), halves_of(x_back)
    smem = pl.BlockSpec(memory_space=pltpu.SMEM)
    vmem = pl.BlockSpec(memory_space=pltpu.VMEM)
    f32 = jnp.float32

    def shape(*dims):
        return jax.ShapeDtypeStruct(dims, f32)

    def scratch(*dims):
        return pltpu.VMEM(dims, f32)

    between = scratch(total, 2, TILE, rows)
    waves_room = scratch(total, 2 * rows, rows)
    send_shape = shape(total, 2, rows, rows)

    turned = vorticity_grid.reshape(rows, rows, total).transpose(2, 1, 0)
    start = pl.pallas_call(
        functools.partial(start_kernel, total, rows),
        out_shape=send_shape,
        in_specs=[vmem] * 2,
        out_specs=vmem,
        scratch_shapes=[waves_room, between],
        compiler_params=params(),
        name="start",
    )(turned, y_forth)

    def product(*flat):
        return pl.pallas_call(
            functools.partial(product_kernel, total, rows, unit),
            out_shape=send_shape,
            in_specs=[smem] + [vmem] * (2 + len(flat)),
            out_specs=vmem,
            scratch_shapes=[
                waves_room, scratch(total, rows, rows), scratch(total, rows, rows), between,
            ],
            compiler_params=params(),
            cost_estimate=pl.CostEstimate(flops=10**10, bytes_accessed=0, transcendentals=0),
            name="product",
        )(info, y_forth, y_back, *flat)

    def spectral(stage, source, *inputs):
        steps = rows // TILE + 1
        count = 3 + stage if stage < 2 else 0
        plain = pl.BlockSpec((total, 2, TILE, rows), lambda i: (0, 0, i, 0))
        main = pl.BlockSpec((total, 2, TILE, rows), lambda i: (0, 0, jnp.maximum(i - 1, 0), 0))
        anywhere = pl.BlockSpec(memory_space=pl.ANY)
        whole = shape(total, 2, rows + TILE, rows)
        fields = shape(own, count, 2, rows, rows)
        if stage < 2:
            outs, out_specs = [whole] * (1 + stage) + [fields], [plain] * (1 + stage) + [anywhere]
        else:
            outs, out_specs = [shape(total, 2, rows, rows)] * 2, [main] * 2
        tables = (twist, *x_forth, *x_back)
        rooms = [
            scratch(total * TILE, 2 * rows), scratch(total * TILE, 2 * rows), between,
            scratch(4, own, TILE, rows), scratch(total, 2, rows, rows),
            pltpu.SemaphoreType.DMA((rows // PART, total)),
            pltpu.SemaphoreType.DMA((rows // PART,)),
            pltpu.SemaphoreType.DMA((1,)),
        ]
        if count:
            rooms += [scratch(own, count, 2, rows, rows)]
            rooms += [pltpu.SemaphoreType.DMA((rows // TILE,))] * 3
        return pl.pallas_call(
            functools.partial(spectral_kernel, total, rows, grid, stage),
            grid=(steps,),
            out_shape=outs,
            in_specs=[smem, smem, anywhere] + [vmem] * len(tables) + [plain] * len(inputs),
            out_specs=out_specs,
            scratch_shapes=rooms,
            compiler_params=pltpu.CompilerParams(
                vmem_limit_bytes=56 * 1024 * 1024, has_side_effects=True
            ),
            cost_estimate=pl.CostEstimate(flops=10**10, bytes_accessed=0, transcendentals=0),
            name=f"spectral{stage}",
        )(info, side, source, *tables, *inputs)

    count_q = -(-half_low // total)
    force = low_spectrum(forcing_grid, rank, total)
    turned_force = jnp.roll(jnp.flip(force, 2), 1, 2) * jnp.array([1.0, -1.0])[None, :, None]
    turned_force = jnp.roll(jnp.flip(turned_force, 0), 1, 0)
    force_all = jnp.concatenate([turned_force, force], 0)
    wave_kx = jnp.arange(LOW, dtype=jnp.int32)[None, None, :] - half_low

    def drive_rows(part, rows_y):
        squares = wave_kx * wave_kx + rows_y * rows_y
        mask = jnp.zeros(squares.shape, bool)
        for index in range(SHELLS):
            radius = forcing_shells[index]
            mask = mask | ((radius * radius <= squares) & (squares < (radius + 1) * (radius + 1)))
        return jnp.where(mask, part, 0.0)

    part = lax.dynamic_slice_in_dim(
        force_all, jnp.clip(first_wave + half_low, 0, LOW - rows), rows, 0
    )
    part = drive_rows(part, first_wave + jnp.arange(rows, dtype=jnp.int32)[:, None, None])
    extra = drive_rows(force[:1], extra_wave)
    extra = jnp.concatenate([extra, jnp.zeros((TILE - 1,) + extra.shape[1:], f32)], 0)
    part = jnp.concatenate([extra, part], 0)
    part = part.reshape(part.shape[0], 2, 2 * count_q, total).transpose(3, 1, 0, 2)
    gap = jnp.zeros(part.shape[:3] + (rows - 2 * count_q,), f32)
    drive = jnp.concatenate([part[..., count_q:], gap, part[..., :count_q]], 3)

    state, fields = spectral(0, start)
    advect = product(fields, start)
    moved, first, fields = spectral(1, advect, state, drive)
    advect = product(fields)
    ahead, now = spectral(2, advect, state, moved, first, drive)
    block = ahead[..., : 2 * count_q]
    spectrum = now.transpose(1, 2, 3, 0).reshape(2, rows, grid)

    part_of = LOW // total
    count_d = -(-half_low // rows)
    signed = np.arange(LOW) - half_low
    spots = np.arange(LOW)
    col_cos, col_sin = (
        t.astype(np.float32) / 16.0 for t in turn(signed[:, None] * spots[None, :], LOW)
    )
    column = np.stack([np.stack([col_cos, col_sin]), np.stack([-col_sin, col_cos])])
    column = column.reshape(2, 2, 2 * count_q, total, LOW)
    mixed = contract("pctq,cdqpa->adt", block, column).reshape(total, part_of, 2, rows)
    mixed = lax.all_to_all(mixed, AXES, split_axis=0, concat_axis=0, tiled=True)
    mixed = jnp.concatenate([mixed[total - count_d :], mixed[:count_d]], 0)
    mixed = mixed.transpose(2, 0, 3, 1).reshape(2, 2 * count_d * rows, part_of)
    coarse = contract("cqa,cqb->ab", mixed, np.stack([col_cos, -col_sin]))
    return (spectrum, coarse)


def solution(mesh):
    placed = (P(AXES, None), P(AXES, None), P(), P())

    def run(vorticity_grid, *rest):
        rows = vorticity_grid.shape[0] // mesh.size
        chosen = body if rows % 128 == 0 and mesh.size >= 8 else narrow_body
        return jax.shard_map(
            chosen,
            mesh=mesh,
            in_specs=placed,
            out_specs=(P(None, AXES, None), P(AXES, None)),
            check_vma=False,
        )(vorticity_grid, *rest)

    return run
```
